32 devices in a mesh: groups: 2 (over x), tile: 16 (over z, y, core).
Axes of the slice: x: 2, y: 2, z: 4, core: 2. Of those that a mesh axis runs over, the one named last changes fastest.
Arguments:
- echoes: float32 [2, 32, 16384], P(None, ('groups', 'tile')), parts along dimension 1, may hold values from -6 to 6
- bin_start: int32 [32, 16], P(('groups', 'tile')), parts along dimension 0, may hold values from 0 to 16128
- bin_fraction: float32 [16, 32], P(None, ('groups', 'tile')), parts along dimension 1, may hold values from 0 to 1
- row_phase: float32 [16, 32, 128], P(None, ('groups', 'tile')), parts along dimension 1, may hold values from -3.140625 to 3.140625
- column_phase: float32 [16, 32, 128], P(None, ('groups', 'tile')), parts along dimension 1, may hold values from -3.140625 to 3.140625
- row_bin: int32 [16, 32, 128], P(None, ('groups', 'tile')), parts along dimension 1, may hold values from 0 to 127
- column_bin: int32 [16, 32, 128], P(None, ('groups', 'tile')), parts along dimension 1, may hold values from 0 to 127
Outputs:
- focused: float32 [2, 32, 128, 128], P(None, ('groups', 'tile')), parts along dimension 1
- correction: float32 [2, 32], P(None, ('groups', 'tile')), parts along dimension 1
The draws below stay inside these ranges and needn't reach their ends.
There are 2 independent parts, one for each index of `groups`. The reference program is written for one: setup_inputs(seed, part) draws one part's arguments, and reference() takes and returns one part's arrays. A program takes and returns all parts, laid end to end along the dimension named above; each array names one. Nothing has to cross between parts.
Inputs may be any that keep to these rules, and one draw needn't show every extreme that they name: The window of 256 range bins that begins at bin_start lies within the 16384 bins.
All inputs are finite; a program needn't handle non-finite values.
Results may differ from the reference program's by a relative error of at most 0.012.
Values may be sent and summed in bfloat16 or wider, within the bound.
A program may use at most 320 MiB of HBM per device.

```python
import math
import jax
import jax.numpy as jnp
from jax import lax

SAMPLES = 16384
ROWS = 128
COLS = 128
BINR = 128
BINC = 128
PULSES = 16
TILES = 16


def plant(result, own_key, low, high):
    longest = result.shape.index(max(result.shape))
    spots = []
    for shift in (0, 1):
        where = [jax.random.randint(jax.random.fold_in(own_key, axis), (), 0, length) for axis, length in enumerate(result.shape)]
        where[longest] = (where[longest] + shift) % result.shape[longest]
        spots.append(tuple(where))
    return result.at[spots[0]].set(low).at[spots[1]].set(high)


def block_levels(key, dims, pieces, low, high):
    factor_of = 1.0
    for dim, parts in pieces:
        draws = jax.random.uniform(jax.random.fold_in(jax.random.fold_in(key, 6), dim), (parts,), jnp.float32, low / len(pieces), high / len(pieces))
        factor_of = factor_of * jnp.repeat(jnp.exp(draws), dims[dim] // parts).reshape((-1,) + (1,) * (len(dims) - 1 - dim))
    return factor_of


def normal_values(stream_key, shape, scale, most, cuts=(), kind=jnp.bfloat16):
    array = scale * jax.random.normal(stream_key, shape, jnp.float32)
    if cuts:
        array = array * block_levels(stream_key, shape, cuts, -0.22, 0.18)
    return jnp.clip(array, -most, most).astype(kind)


def setup_inputs(seed: int = 0, part: int = 0) -> dict:
    keys = jax.random.split(jax.random.key(seed), 8)
    part_keys = jax.random.split(jax.random.fold_in(keys[7], part), 8)
    return {
        "echoes": normal_values(part_keys[0], (2, PULSES, SAMPLES), 1.0, 6.0, ((1, 16),), jnp.float32),
        "bin_start": plant(jax.random.randint(part_keys[1], (PULSES, TILES), 0, SAMPLES - BINR - BINC + 1), jax.random.fold_in(part_keys[1], 1), 0, SAMPLES - BINR - BINC).astype(jnp.int32),
        "bin_fraction": jnp.clip(1.0 * jax.random.uniform(part_keys[2], (PULSES, TILES), jnp.float32) ** block_levels(part_keys[2], (PULSES, TILES), ((1, 16),), -0.2, 0.2), 0.0, 1.0),
        "row_phase": jnp.clip(jax.random.uniform(part_keys[3], (PULSES, TILES, ROWS), jnp.float32, -3.140625, 3.140625), -3.140625, 3.140625),
        "column_phase": jnp.clip(jax.random.uniform(part_keys[4], (PULSES, TILES, COLS), jnp.float32, -3.140625, 3.140625), -3.140625, 3.140625),
        "row_bin": plant(jax.random.randint(part_keys[5], (PULSES, TILES, ROWS), 0, BINR), jax.random.fold_in(part_keys[5], 1), 0, BINR - 1).astype(jnp.int32),
        "column_bin": plant(jax.random.randint(part_keys[6], (PULSES, TILES, COLS), 0, BINC), jax.random.fold_in(part_keys[6], 1), 0, BINC - 1).astype(jnp.int32),
    }


def rounded(values):
    return lax.optimization_barrier(values.astype(jnp.bfloat16)).astype(jnp.float32)

def normalize(real_part, imag_part):
    magnitude = real_part * real_part + imag_part * imag_part
    denominator = jnp.sqrt(magnitude + jnp.mean(magnitude) + 1e-06)
    return (real_part / denominator, imag_part / denominator)

def reference(echoes, bin_start, bin_fraction, row_phase, column_phase, row_bin, column_bin):
    signal = echoes[0] + 1j * echoes[1]
    spectrum = jnp.fft.fft(signal, axis=1) / math.sqrt(SAMPLES)
    spectra = rounded(jnp.stack([jnp.real(spectrum), jnp.imag(spectrum)]))
    window_len = BINR + BINC
    offsets = jnp.arange(window_len, dtype=jnp.int32)
    shifts = jnp.arange(BINC, dtype=jnp.int32)
    norm_scale = 1.0 / math.sqrt(PULSES)
    pulse_ids = jnp.arange(PULSES, dtype=jnp.int32)

    def contribution(pulse_id):
        begins = bin_start[pulse_id][:, None] + offsets[None, :]
        window = spectra[:, pulse_id][:, begins]
        weight_frac = bin_fraction[pulse_id][None, :, None]
        profile = rounded((1.0 - weight_frac) * window[..., :-1] + weight_frac * window[..., 1:])
        index_rows = (row_bin[pulse_id][:, :, None] + shifts[None, None, :]).reshape(TILES, ROWS * BINC)
        chosen_real = jnp.take_along_axis(profile[0], index_rows, axis=1).reshape(TILES, ROWS, BINC)
        chosen_imag = jnp.take_along_axis(profile[1], index_rows, axis=1).reshape(TILES, ROWS, BINC)
        row_cosine = rounded(jnp.cos(row_phase[pulse_id]))[:, :, None]
        row_sine = rounded(jnp.sin(row_phase[pulse_id]))[:, :, None]
        steer_real = rounded(row_cosine * chosen_real - row_sine * chosen_imag)
        steer_imag = rounded(row_cosine * chosen_imag + row_sine * chosen_real)
        index_columns = jnp.broadcast_to(column_bin[pulse_id][:, None, :], (TILES, ROWS, COLS))
        moved_real = jnp.take_along_axis(steer_real, index_columns, axis=2)
        moved_imag = jnp.take_along_axis(steer_imag, index_columns, axis=2)
        column_cosine = rounded(jnp.cos(column_phase[pulse_id]))[:, None, :]
        column_sine = rounded(jnp.sin(column_phase[pulse_id]))[:, None, :]
        return (column_cosine * moved_real - column_sine * moved_imag, column_cosine * moved_imag + column_sine * moved_real)

    def image_of(weight_real, weight_imag):

        def visit_pulse(running, pulse_id):
            part_real, part_imag = contribution(pulse_id)
            new_real = running[0] + weight_real[pulse_id] * part_real - weight_imag[pulse_id] * part_imag
            new_imag = running[1] + weight_real[pulse_id] * part_imag + weight_imag[pulse_id] * part_real
            return ((new_real, new_imag), None)
        zero_image = jnp.zeros((TILES, ROWS, COLS), jnp.float32)
        (image_real, image_imag), _ = lax.scan(visit_pulse, (zero_image, zero_image), pulse_ids)
        return (image_real * norm_scale, image_imag * norm_scale)

    def correlate(image_real, image_imag):

        def visit_pulse(running, pulse_id):
            part_real, part_imag = contribution(pulse_id)
            totals = (jnp.sum(part_real * image_real + part_imag * image_imag), jnp.sum(part_real * image_imag - part_imag * image_real), jnp.sum(part_real * part_real + part_imag * part_imag))
            return (running, totals)
        _, totals = lax.scan(visit_pulse, jnp.zeros((), jnp.float32), pulse_ids)
        return totals
    unit_weights = jnp.ones((PULSES,), jnp.float32)
    zero_weights = jnp.zeros((PULSES,), jnp.float32)
    first_real, first_imag = image_of(unit_weights, zero_weights)
    cross_real, cross_imag, energy = correlate(first_real, first_imag)
    one_real, one_imag = normalize(cross_real - energy * norm_scale, cross_imag)
    second_real, second_imag = image_of(one_real, one_imag)
    cross_real, cross_imag, _ = correlate(second_real, second_imag)
    rest_real = cross_real - one_real * energy * norm_scale
    rest_imag = cross_imag - one_imag * energy * norm_scale
    again_real = one_real * rest_real + one_imag * rest_imag
    again_imag = one_real * rest_imag - one_imag * rest_real
    two_real, two_imag = normalize(again_real, again_imag)
    total_real = one_real * two_real - one_imag * two_imag
    total_imag = one_real * two_imag + one_imag * two_real
    final_real, final_imag = image_of(total_real, total_imag)
    return (jnp.stack([final_real, final_imag]), jnp.stack([total_real, total_imag]))
```

```python
import functools
import math

import jax
import jax.numpy as jnp
import numpy as np
from jax import lax
from jax.experimental import pallas as pl
from jax.experimental.pallas import tpu as pltpu
from jax.sharding import PartitionSpec as P

LANES = 128
OCTET = 8
MESH = pl.DeviceIdType.MESH
F32 = jnp.float32
BF16 = jnp.bfloat16


def tables(samples):
    inner = LANES
    outer = samples // inner

    def wave(rows, columns, period):
        product = np.arange(rows)[:, None] * np.arange(columns)[None, :] % period
        phases = product * (2.0 * np.pi / period)
        return np.cos(phases), np.sin(phases)

    def split(table):
        table = table.astype(np.float32)
        high = table.astype(jnp.bfloat16)
        low = (table - high.astype(np.float32)).astype(jnp.bfloat16)
        return np.stack([high, low])

    first = split(np.concatenate(wave(outer, outer, outer), 1))
    last = split(np.concatenate(wave(inner, inner, inner), 1))
    turn = np.stack(wave(outer, inner, samples)) / math.sqrt(samples)
    return first, turn.astype(np.float32), last


def dot(a, b, dims=((1,), (0,)), precision=None):
    return lax.dot_general(a, b, (dims, ((), ())), precision=precision, preferred_element_type=F32)


def split3(table_ref, data, dims):
    high = data.astype(BF16)
    low = (data - high.astype(F32)).astype(BF16)
    return dot(table_ref[0], high, dims) + (dot(table_ref[1], high, dims) + dot(table_ref[0], low, dims))


def normalize(real_part, imag_part, axis, count):
    magnitude = real_part * real_part + imag_part * imag_part
    mean = jnp.sum(magnitude, axis=axis, keepdims=True) / count
    denominator = jnp.sqrt(magnitude + mean + 1e-06)
    return real_part / denominator, imag_part / denominator


def pick(source, index):
    numbers = lax.GatherDimensionNumbers(
        offset_dims=(), collapsed_slice_dims=(1,), start_index_map=(1,),
        operand_batching_dims=(0,), start_indices_batching_dims=(0,),
    )
    return lax.gather(
        source, index[..., None], numbers, (1, 1), mode=lax.GatherScatterMode.PROMISE_IN_BOUNDS
    )


def kernel(
    n, starts_in, echo_in, first_in, turn_in, last_in, row_phase_in, column_phase_in, row_bin_in, column_bin_in,
    fraction_in,
    focused, correction,
    starts, echo, first, turn, last, row_phase, column_phase, row_bin, column_bin, fraction, in_sem,
    spec, outgoing, gathered, waves, bins_of, share, index_low, index_all, steer, windows, parts,
    gram_rows, message, messages,
    send_sem, recv_sem, send_sem2, recv_sem2,
):
    me = lax.axis_index("tile")
    rows = row_phase.shape[2]
    scale = 1.0 / math.sqrt(n)
    groups = n // OCTET
    mine = me // OCTET
    pair = 2 * n

    def group_of(slot):
        return lax.rem(mine + slot, groups)

    barrier = pltpu.get_barrier_semaphore()
    for k in range(1, n):
        pl.semaphore_signal(barrier, inc=1, device_id={"tile": lax.rem(me + k, n)}, device_id_type=MESH)

    sources = (
        starts_in, echo_in, first_in, turn_in, last_in, row_phase_in, column_phase_in, row_bin_in, column_bin_in,
        fraction_in,
    )
    targets = (starts, echo, first, turn, last, row_phase, column_phase, row_bin, column_bin, fraction)
    loads = [
        pltpu.make_async_copy(source, target, in_sem.at[i])
        for i, (source, target) in enumerate(zip(sources, targets))
    ]
    for load in loads[1:] + loads[:1]:
        load.start()

    upper = (2 * me) // n

    def other(k):
        place = upper * k + (1 - upper) * (n - 2 - k)
        return place + (place >= me).astype(jnp.int32)


    loads[1].wait()
    loads[2].wait()
    real, imag = echo[0], echo[1]
    data = jnp.concatenate(
        [jnp.concatenate([real, imag], 1), jnp.concatenate([imag, -real], 1)], 0
    )
    section = split3(first, data, ((1,), (0,)))
    half = section.shape[1] // 2
    loads[3].wait()
    loads[4].wait()
    real, imag = section[:, :half], section[:, half:]
    turned_real = real * turn[0] + imag * turn[1]
    turned_imag = imag * turn[0] - real * turn[1]
    data = jnp.concatenate(
        [jnp.concatenate([turned_real, turned_imag], 1), jnp.concatenate([turned_imag, -turned_real], 1)], 0
    )
    spectrum = split3(last, data, ((1,), (1,)))
    bins = spectrum.shape[0]
    spectrum = spectrum.astype(BF16).astype(F32)
    for h in range(2):
        spec[h, 0:bins, :] = spectrum[:, h * LANES : (h + 1) * LANES]
        spec[h, bins:, :] = jnp.zeros((spec.shape[1] - bins, LANES), F32)

    lane = lax.broadcasted_iota(jnp.int32, (OCTET, LANES), 1)
    loads[0].wait()
    for t in range(n):
        start = starts[0, t]
        top = start // LANES
        left = LANES - start % LANES
        pieces = []
        for h in range(2):
            moved = pltpu.roll(spec[h, pl.ds(top, OCTET), :], left % LANES, 1)
            below = pltpu.roll(moved, OCTET - 1, 0)
            pieces.append(jnp.where(lane < left, moved, below)[0:2])
        outgoing[t] = jnp.concatenate(pieces, 0).astype(BF16)

    pl.semaphore_wait(barrier, n - 1)

    def window_copy(device, slot):
        return pltpu.make_async_remote_copy(
            src_ref=outgoing.at[device],
            dst_ref=gathered.at[slot],
            send_sem=send_sem.at[device],
            recv_sem=recv_sem.at[slot],
            device_id={"tile": device},
            device_id_type=MESH,
        )

    for k in range(n - 1):
        window_copy(other(k), me).start()
    gathered[me] = outgoing[me]

    def rounded(values):
        return values.astype(BF16).astype(F32)

    for load in loads[5:]:
        load.wait()

    def by_octets(values):
        return values.reshape(groups, OCTET, LANES)

    angles = row_phase[:, 0, :]
    waves[0] = by_octets(rounded(jnp.cos(angles)))
    waves[1] = by_octets(rounded(jnp.sin(angles)))
    angles = column_phase[:, 0, :]
    waves[2] = by_octets(rounded(jnp.cos(angles)))
    waves[3] = by_octets(rounded(jnp.sin(angles)))
    bins_of[0] = by_octets(row_bin[:, 0, :])
    bins_of[1] = by_octets(column_bin[:, 0, :])
    octet_id = lax.broadcasted_iota(jnp.int32, (OCTET, LANES), 0)
    tiles = rows // OCTET

    def spread(values, u):
        return jnp.broadcast_to(values[:, u : u + 1], (OCTET, LANES))

    for slot in range(groups):
        group = group_of(slot)
        part = jnp.zeros((OCTET, LANES), F32)
        for i in range(OCTET):
            part = jnp.where(octet_id == i, fraction[0, group * OCTET + i], part)
        share[slot] = part
        row_cosine, row_sine = waves[0, group], waves[1, group]
        column_cosine, column_sine = waves[2, group], waves[3, group]
        row_index, column_index = bins_of[0, group], bins_of[1, group]
        for u in range(rows):
            cosine, sine = spread(row_cosine, u), spread(row_sine, u)
            index = spread(row_index, u) + column_index
            index_all[slot, u] = index
            index_low[slot, u] = index & (LANES - 1)
            steer[0, slot, u] = cosine * column_cosine - sine * column_sine
            steer[1, slot, u] = cosine * column_sine + sine * column_cosine

    def contribute(slot):
        group = group_of(slot)
        for i in range(OCTET):
            windows[slot, 4 * i : 4 * (i + 1), :] = gathered[group * OCTET + i].astype(F32)
        window = [windows[slot, pl.ds(q, OCTET, stride=4), :] for q in range(4)]
        moved = [pltpu.roll(values, LANES - 1, 1) for values in window]
        fraction_of = share[slot]
        profile = []
        for q in range(4):
            shifted = moved[q] if q % 2 else jnp.where(lane == LANES - 1, moved[q + 1], moved[q])
            profile.append(rounded((1.0 - fraction_of) * window[q] + fraction_of * shifted))
        for u in range(rows):
            low = index_low[slot, u]
            is_low = index_all[slot, u] < LANES
            real = jnp.where(is_low, pick(profile[0], low), pick(profile[1], low))
            imag = jnp.where(is_low, pick(profile[2], low), pick(profile[3], low))
            turn_real, turn_imag = steer[0, slot, u], steer[1, slot, u]
            both = jnp.concatenate([turn_real * real - turn_imag * imag, turn_real * imag + turn_imag * real], 0)
            top = (u % OCTET) * pair + slot * 2 * OCTET
            left = (u // OCTET) * LANES
            parts[top : top + 2 * OCTET, left : left + LANES] = both.astype(BF16)

    for slot in range(groups):
        for k in range(1 if slot == 0 else 0, OCTET):
            device = group_of(slot) * OCTET + lax.rem(me + k, OCTET)
            window_copy(device, device).wait_recv()
        contribute(slot)

    total = None
    for top in range(0, OCTET * pair, LANES):
        values = parts[top : top + LANES, :]
        product = dot(values, values, ((1,), (1,)))
        total = product if total is None else total + product
    gram = total[0:pair]
    for i in range(1, LANES // pair):
        gram = gram + pltpu.roll(total[i * pair : (i + 1) * pair], LANES - i * pair, 1)
    imag_lane = (lane // OCTET) % 2 == 1
    for slot in range(groups):
        top = slot * 2 * OCTET
        real, imag = gram[top : top + OCTET], gram[top + OCTET : top + 2 * OCTET]
        values = real + jnp.where(
            imag_lane, -pltpu.roll(imag, OCTET, 1), pltpu.roll(imag, LANES - OCTET, 1)
        )
        values = jnp.where(lane < pair, values, 0.0)
        width = pair
        while width < LANES:
            values = values + pltpu.roll(values, width, 1)
            width *= 2
        gram_rows[group_of(slot)] = pltpu.roll(values, 2 * OCTET * mine, 1)
    full = gram_rows[...].reshape(n, LANES)
    depth = n * pair // LANES
    folds = LANES // pair
    block_id = lax.broadcasted_iota(jnp.int32, (depth, LANES), 1) // pair
    packed = full[0:depth]
    for j in range(1, folds):
        packed = jnp.where(block_id == j, full[j * depth : (j + 1) * depth], packed)
    message[...] = packed
    messages[me] = packed

    def gram_copy(device, slot):
        return pltpu.make_async_remote_copy(
            src_ref=message,
            dst_ref=messages.at[slot],
            send_sem=send_sem2.at[device],
            recv_sem=recv_sem2.at[slot],
            device_id={"tile": device},
            device_id_type=MESH,
        )

    for k in range(n - 1):
        gram_copy(other(k), me).start()
    for k in range(n - 1):
        window_copy(other(k), me).wait_send()
    for k in reversed(range(n - 1)):
        gram_copy(other(k), other(k)).wait_recv()

    total = jnp.sum(messages[...], axis=0)
    gram = jnp.concatenate([total] + [pltpu.roll(total, LANES - j * pair, 1) for j in range(1, folds)], 0)
    row_id = lax.broadcasted_iota(jnp.int32, gram.shape, 0)
    lane_id = lax.broadcasted_iota(jnp.int32, gram.shape, 1)
    column_id = lane_id // (2 * OCTET) * OCTET + lane_id % OCTET
    off_diagonal = (lane_id < pair) & (lane_id // OCTET % 2 == 0) & (column_id != row_id)
    gram_real = jnp.where(off_diagonal, gram * scale, 0.0)
    gram_imag = jnp.where(off_diagonal, pltpu.roll(gram, LANES - OCTET, 1) * scale, 0.0)

    def along(values, axis):
        return jnp.sum(values, axis=axis, keepdims=True)

    one_real, one_imag = normalize(along(gram_real, 1), along(gram_imag, 1), 0, n)
    row_real, row_imag = normalize(along(gram_real, 0), -along(gram_imag, 0), 1, n)
    rest_real = along(gram_real * one_real + gram_imag * one_imag, 0)
    rest_imag = along(gram_real * one_imag - gram_imag * one_real, 0)
    again_real = row_real * rest_real + row_imag * rest_imag
    again_imag = row_real * rest_imag - row_imag * rest_real
    two_real, two_imag = normalize(again_real, again_imag, 1, n)
    total_real = row_real * two_real - row_imag * two_imag
    total_imag = row_real * two_imag + row_imag * two_real
    lane_row = lax.broadcasted_iota(jnp.int32, total_real.shape, 1)
    own_lane = (me // OCTET) * 2 * OCTET + me % OCTET
    own = lane_row == own_lane
    correction[...] = jnp.concatenate(
        [along(jnp.where(own, total_real, 0.0), 1), along(jnp.where(own, total_imag, 0.0), 1)], 1
    )
    row_parts = (lane_row // OCTET) % 2 == 1
    weights = []
    for values in (
        jnp.where(row_parts, -pltpu.roll(total_imag, OCTET, 1), total_real),
        jnp.where(row_parts, pltpu.roll(total_real, OCTET, 1), total_imag),
    ):
        values = jnp.where(lane_row < pair, values * scale, 0.0)
        width = pair
        while width < LANES:
            values = values + pltpu.roll(values, width, 1)
            width *= 2
        values = pltpu.roll(values, LANES - 2 * OCTET * mine, 1)
        weights.append(jnp.broadcast_to(values, (OCTET, LANES)))
    weights = jnp.concatenate(weights, 0)
    phase_id = lax.broadcasted_iota(jnp.int32, weights.shape, 0) % OCTET
    weight_lane = lax.broadcasted_iota(jnp.int32, weights.shape, 1)
    spans = [
        jnp.where((weight_lane + left) // pair == phase_id, weights, 0.0) for left in range(0, OCTET * pair, LANES)
    ]
    weights = jnp.concatenate(spans, 1)
    high = weights.astype(BF16)
    low = (weights - high.astype(F32)).astype(BF16)
    weights = jnp.concatenate([high, low], 0)
    step = 2 * LANES
    for left in range(0, tiles * LANES, step):
        image = dot(weights, parts[:, left : left + step])
        image = image[0 : 2 * OCTET] + image[2 * OCTET :]
        for i in range(step // LANES):
            t = left // LANES + i
            span = slice(t * OCTET, (t + 1) * OCTET)
            for h in range(2):
                focused[h, 0, span, :] = image[h * OCTET : (h + 1) * OCTET, i * LANES : (i + 1) * LANES]

    for k in range(n - 1):
        gram_copy(other(k), me).wait_send()


def solution(mesh):
    n = mesh.shape["tile"]

    def per_device(echoes, bin_start, bin_fraction, row_phase, column_phase, row_bin, column_bin):
        samples = echoes.shape[2]
        rows, columns = row_phase.shape[2], column_phase.shape[2]
        first, turn, last = tables(samples)
        bins = samples // LANES
        echo = echoes.reshape(2, bins, LANES)
        vmem = pl.BlockSpec(memory_space=pltpu.VMEM)
        operands = (
            bin_start, echo, jnp.asarray(first), jnp.asarray(turn), jnp.asarray(last),
            row_phase, column_phase, row_bin, column_bin, bin_fraction.T,
        )
        depth = n * 2 * n // LANES
        focused, correction = pl.pallas_call(
            functools.partial(kernel, n),
            out_shape=(
                pltpu.VMEM((2, 1, rows, columns), F32),
                pltpu.VMEM((1, 2), F32),
            ),
            in_specs=[pl.BlockSpec(memory_space=pltpu.HBM)] * len(operands),
            out_specs=(vmem, vmem),
            scratch_shapes=[pltpu.SMEM(bin_start.shape, jnp.int32)]
            + [pltpu.VMEM(operand.shape, operand.dtype) for operand in operands[1:9]]
            + [pltpu.SMEM((1, n), F32), pltpu.SemaphoreType.DMA((len(operands),))]
            + [
                pltpu.VMEM((2, bins + OCTET, LANES), F32),
                pltpu.VMEM((n, 4, LANES), BF16),
                pltpu.VMEM((n, 4, LANES), BF16),
                pltpu.VMEM((4, n // OCTET, OCTET, LANES), F32),
                pltpu.VMEM((2, n // OCTET, OCTET, LANES), jnp.int32),
                pltpu.VMEM((n // OCTET, OCTET, LANES), F32),
                pltpu.VMEM((n // OCTET, rows, OCTET, LANES), jnp.int32),
                pltpu.VMEM((n // OCTET, rows, OCTET, LANES), jnp.int32),
                pltpu.VMEM((2, n // OCTET, rows, OCTET, LANES), F32),
                pltpu.VMEM((n // OCTET, 4 * OCTET, LANES), F32),
                pltpu.VMEM((OCTET * 2 * n, rows // OCTET * columns), BF16),
                pltpu.VMEM((n // OCTET, OCTET, LANES), F32),
                pltpu.VMEM((depth, LANES), F32),
                pltpu.VMEM((n, depth, LANES), F32),
                pltpu.SemaphoreType.DMA((n,)),
                pltpu.SemaphoreType.DMA((n,)),
                pltpu.SemaphoreType.DMA((n,)),
                pltpu.SemaphoreType.DMA((n,)),
            ],
            compiler_params=pltpu.CompilerParams(collective_id=0, has_side_effects=True),
        )(*operands)
        return focused, correction.T

    split = ("groups", "tile")
    in_specs = (
        P(None, split, None),
        P(split, None),
        P(None, split),
        P(None, split, None),
        P(None, split, None),
        P(None, split, None),
        P(None, split, None),
    )
    out_specs = (P(None, split, None, None), P(None, split))
    return jax.shard_map(per_device, mesh=mesh, in_specs=in_specs, out_specs=out_specs, check_vma=False)
```

```python
import functools
import math

import jax
import jax.numpy as jnp
import numpy as np
from jax import lax
from jax.experimental import pallas as pl
from jax.experimental.pallas import tpu as pltpu
from jax.sharding import PartitionSpec as P

LANES = 128
OCTET = 8
MESH = pl.DeviceIdType.MESH
F32 = jnp.float32
BF16 = jnp.bfloat16


def tables(samples):
    inner = LANES
    outer = samples // inner

    def wave(rows, columns, period):
        product = np.arange(rows)[:, None] * np.arange(columns)[None, :] % period
        phases = product * (2.0 * np.pi / period)
        return np.cos(phases), np.sin(phases)

    def split(table):
        table = table.astype(np.float32)
        high = table.astype(jnp.bfloat16)
        low = (table - high.astype(np.float32)).astype(jnp.bfloat16)
        return np.stack([high, low])

    first = split(np.concatenate(wave(outer, outer, outer), 1))
    last = split(np.concatenate(wave(inner, inner, inner), 1))
    turn = np.stack(wave(outer, inner, samples)) / math.sqrt(samples)
    return first, turn.astype(np.float32), last


def dot(a, b, dims=((1,), (0,)), precision=None):
    return lax.dot_general(a, b, (dims, ((), ())), precision=precision, preferred_element_type=F32)


def split3(table_ref, data, dims):
    high = data.astype(BF16)
    low = (data - high.astype(F32)).astype(BF16)
    return dot(table_ref[0], high, dims) + (dot(table_ref[1], high, dims) + dot(table_ref[0], low, dims))


def normalize(real_part, imag_part, axis, count):
    magnitude = real_part * real_part + imag_part * imag_part
    mean = jnp.sum(magnitude, axis=axis, keepdims=True) / count
    denominator = jnp.sqrt(magnitude + mean + 1e-06)
    return real_part / denominator, imag_part / denominator


def pick(source, index):
    numbers = lax.GatherDimensionNumbers(
        offset_dims=(), collapsed_slice_dims=(1,), start_index_map=(1,),
        operand_batching_dims=(0,), start_indices_batching_dims=(0,),
    )
    return lax.gather(
        source, index[..., None], numbers, (1, 1), mode=lax.GatherScatterMode.PROMISE_IN_BOUNDS
    )


def kernel(
    n, starts_in, echo_in, first_in, turn_in, last_in, row_phase_in, column_phase_in, row_bin_in, column_bin_in,
    fraction_in,
    parts, weights_out, correction,
    starts, echo, first, turn, last, row_phase, column_phase, row_bin, column_bin, fraction, in_sem,
    spec, outgoing, gathered, waves, share, index_all, steer, windows,
    gram_rows, message, messages,
    send_sem, recv_sem, send_sem2, recv_sem2,
):
    me = lax.axis_index("tile")
    rows = row_phase.shape[2]
    scale = 1.0 / math.sqrt(n)
    groups = n // OCTET
    mine = me // OCTET
    pair = 2 * n

    def group_of(slot):
        return lax.rem(mine + slot, groups)

    barrier = pltpu.get_barrier_semaphore()
    for k in range(1, n):
        pl.semaphore_signal(barrier, inc=1, device_id={"tile": lax.rem(me + k, n)}, device_id_type=MESH)

    sources = (
        starts_in, echo_in, first_in, turn_in, last_in, row_phase_in, column_phase_in, row_bin_in, column_bin_in,
        fraction_in,
    )
    targets = (starts, echo, first, turn, last, row_phase, column_phase, row_bin, column_bin, fraction)
    loads = [
        pltpu.make_async_copy(source, target, in_sem.at[i])
        for i, (source, target) in enumerate(zip(sources, targets))
    ]
    for load in loads[1:] + loads[:1]:
        load.start()

    upper = (2 * me) // n

    def other(k):
        place = upper * k + (1 - upper) * (n - 2 - k)
        return place + (place >= me).astype(jnp.int32)


    loads[1].wait()
    loads[2].wait()
    real, imag = echo[0], echo[1]
    data = jnp.concatenate(
        [jnp.concatenate([real, imag], 1), jnp.concatenate([imag, -real], 1)], 0
    )
    section = split3(first, data, ((1,), (0,)))
    half = section.shape[1] // 2
    loads[3].wait()
    loads[4].wait()
    real, imag = section[:, :half], section[:, half:]
    turned_real = real * turn[0] + imag * turn[1]
    turned_imag = imag * turn[0] - real * turn[1]
    data = jnp.concatenate(
        [jnp.concatenate([turned_real, turned_imag], 1), jnp.concatenate([turned_imag, -turned_real], 1)], 0
    )
    spectrum = split3(last, data, ((1,), (1,)))
    bins = spectrum.shape[0]
    spectrum = spectrum.astype(BF16).astype(F32)
    for h in range(2):
        spec[h, 0:bins, :] = spectrum[:, h * LANES : (h + 1) * LANES]
        spec[h, bins:, :] = jnp.zeros((spec.shape[1] - bins, LANES), F32)

    lane = lax.broadcasted_iota(jnp.int32, (OCTET, LANES), 1)
    loads[0].wait()
    for t in range(n):
        start = starts[0, t]
        top = start // LANES
        left = LANES - start % LANES
        pieces = []
        for h in range(2):
            moved = pltpu.roll(spec[h, pl.ds(top, OCTET), :], left % LANES, 1)
            below = pltpu.roll(moved, OCTET - 1, 0)
            pieces.append(jnp.where(lane < left, moved, below)[0:2])
        outgoing[t] = jnp.concatenate(pieces, 0).astype(BF16)

    pl.semaphore_wait(barrier, n - 1)

    def window_copy(device, slot):
        return pltpu.make_async_remote_copy(
            src_ref=outgoing.at[device],
            dst_ref=gathered.at[slot],
            send_sem=send_sem,
            recv_sem=recv_sem.at[slot // OCTET],
            device_id={"tile": device},
            device_id_type=MESH,
        )

    for k in range(n - 1):
        window_copy(other(k), me).start()
    pltpu.make_async_copy(outgoing.at[me], gathered.at[me], recv_sem.at[mine]).start()

    def rounded(values):
        return values.astype(BF16).astype(F32)

    for load in loads[5:]:
        load.wait()

    def by_octets(values):
        return values.reshape(groups, OCTET, LANES)

    angles = row_phase[:, 0, :]
    waves[0] = by_octets(rounded(jnp.cos(angles)))
    waves[1] = by_octets(rounded(jnp.sin(angles)))
    angles = column_phase[:, 0, :]
    waves[2] = by_octets(rounded(jnp.cos(angles)))
    waves[3] = by_octets(rounded(jnp.sin(angles)))
    waves[4] = by_octets(row_bin[:, 0, :].astype(F32))
    waves[5] = by_octets(column_bin[:, 0, :].astype(F32))
    octet_id = lax.broadcasted_iota(jnp.int32, (OCTET, LANES), 0)
    tiles = rows // OCTET

    def spread(values, u):
        return jnp.broadcast_to(values[:, u : u + 1], (OCTET, LANES))

    tables = []
    for slot in range(groups):
        group = group_of(slot)
        part = jnp.zeros((OCTET, LANES), F32)
        for i in range(OCTET):
            part = jnp.where(octet_id == i, fraction[0, group * OCTET + i], part)
        share[slot] = part
        tables.append([rounded(waves[q, group]) for q in range(6)])
    column_bin_of = [table[5].astype(jnp.int32) for table in tables]
    for u in range(rows):
        turns = [(spread(table[0], u), spread(table[1], u)) for table in tables]
        offsets = [spread(table[4], u) for table in tables]
        for slot, ((cosine, sine), offset, table) in enumerate(zip(turns, offsets, tables)):
            column_cosine, column_sine = table[2], table[3]
            offset = offset.astype(jnp.int32)
            index_all[0, slot, u] = (offset + column_bin_of[slot]) & (LANES - 1)
            index_all[1, slot, u] = offset
            steer[0, slot, u] = cosine * column_cosine - sine * column_sine
            steer[1, slot, u] = cosine * column_sine + sine * column_cosine

    def contribute(slot):
        group = group_of(slot)
        for i in range(OCTET):
            windows[slot, 4 * i : 4 * (i + 1), :] = gathered[group * OCTET + i].astype(F32)
        window = [windows[slot, pl.ds(q, OCTET, stride=4), :] for q in range(4)]
        moved = [pltpu.roll(values, LANES - 1, 1) for values in window]
        fraction_of = share[slot]
        profile = []
        for q in range(4):
            shifted = moved[q] if q % 2 else jnp.where(lane == LANES - 1, moved[q + 1], moved[q])
            profile.append(rounded((1.0 - fraction_of) * window[q] + fraction_of * shifted))
        for u in range(rows):
            low = index_all[0, slot, u]
            is_low = index_all[1, slot, u] <= lane
            real = pick(jnp.where(is_low, profile[0], profile[1]), low)
            imag = pick(jnp.where(is_low, profile[2], profile[3]), low)
            turn_real, turn_imag = steer[0, slot, u], steer[1, slot, u]
            both = jnp.concatenate([turn_real * real - turn_imag * imag, turn_real * imag + turn_imag * real], 0)
            top = pl.multiple_of((u % OCTET) * pair + slot * 2 * OCTET, 2 * OCTET)
            left = (u // OCTET) * LANES
            parts[pl.ds(top, 2 * OCTET), left : left + LANES] = both.astype(BF16)

    def visit(slot, carry):
        arrived = gathered.at[pl.ds(group_of(slot) * OCTET, OCTET)]
        pltpu.make_async_copy(arrived, arrived, recv_sem.at[group_of(slot)]).wait()
        contribute(slot)
        return carry

    lax.fori_loop(0, groups, visit, 0)

    total = None
    for top in range(0, OCTET * pair, 2 * LANES):
        values = parts[top : top + 2 * LANES, :]
        product = dot(values, values, ((1,), (1,)))
        product = product[:LANES, :LANES] + product[LANES:, LANES:]
        total = product if total is None else total + product
    gram = total[0:pair]
    for i in range(1, LANES // pair):
        gram = gram + pltpu.roll(total[i * pair : (i + 1) * pair], LANES - i * pair, 1)
    imag_lane = (lane // OCTET) % 2 == 1
    for slot in range(groups):
        top = slot * 2 * OCTET
        real, imag = gram[top : top + OCTET], gram[top + OCTET : top + 2 * OCTET]
        values = real + jnp.where(
            imag_lane, -pltpu.roll(imag, OCTET, 1), pltpu.roll(imag, LANES - OCTET, 1)
        )
        values = jnp.where(lane < pair, values, 0.0)
        width = pair
        while width < LANES:
            values = values + pltpu.roll(values, width, 1)
            width *= 2
        gram_rows[group_of(slot)] = pltpu.roll(values, 2 * OCTET * mine, 1)
    full = gram_rows[...].reshape(n, LANES)
    depth = n * pair // LANES
    folds = LANES // pair
    block_id = lax.broadcasted_iota(jnp.int32, (depth, LANES), 1) // pair
    packed = full[0:depth]
    for j in range(1, folds):
        packed = jnp.where(block_id == j, full[j * depth : (j + 1) * depth], packed)
    message[...] = packed
    messages[me] = packed

    def gram_copy(device, slot):
        return pltpu.make_async_remote_copy(
            src_ref=message,
            dst_ref=messages.at[slot],
            send_sem=send_sem2,
            recv_sem=recv_sem2,
            device_id={"tile": device},
            device_id_type=MESH,
        )

    for k in range(n - 1):
        gram_copy(other(k), me).start()
    sent = outgoing.at[pl.ds(0, n - 1)]
    pltpu.make_async_copy(sent, sent, send_sem).wait()
    sent = messages.at[pl.ds(0, n - 1)]
    pltpu.make_async_copy(sent, sent, recv_sem2).wait()

    total = jnp.sum(messages[...], axis=0)
    gram = jnp.concatenate([total] + [pltpu.roll(total, LANES - j * pair, 1) for j in range(1, folds)], 0)
    row_id = lax.broadcasted_iota(jnp.int32, gram.shape, 0)
    lane_id = lax.broadcasted_iota(jnp.int32, gram.shape, 1)
    column_id = lane_id // (2 * OCTET) * OCTET + lane_id % OCTET
    off_diagonal = (lane_id < pair) & (lane_id // OCTET % 2 == 0) & (column_id != row_id)
    gram_real = jnp.where(off_diagonal, gram * scale, 0.0)
    gram_imag = jnp.where(off_diagonal, pltpu.roll(gram, LANES - OCTET, 1) * scale, 0.0)

    def along(values, axis):
        return jnp.sum(values, axis=axis, keepdims=True)

    one_real, one_imag = normalize(along(gram_real, 1), along(gram_imag, 1), 0, n)
    row_real, row_imag = normalize(along(gram_real, 0), -along(gram_imag, 0), 1, n)
    rest_real = along(gram_real * one_real + gram_imag * one_imag, 0)
    rest_imag = along(gram_real * one_imag - gram_imag * one_real, 0)
    again_real = row_real * rest_real + row_imag * rest_imag
    again_imag = row_real * rest_imag - row_imag * rest_real
    two_real, two_imag = normalize(again_real, again_imag, 1, n)
    total_real = row_real * two_real - row_imag * two_imag
    total_imag = row_real * two_imag + row_imag * two_real
    lane_row = lax.broadcasted_iota(jnp.int32, total_real.shape, 1)
    own_lane = (me // OCTET) * 2 * OCTET + me % OCTET
    own = lane_row == own_lane
    correction[...] = jnp.concatenate(
        [along(jnp.where(own, total_real, 0.0), 1), along(jnp.where(own, total_imag, 0.0), 1)], 1
    )
    row_parts = (lane_row // OCTET) % 2 == 1
    weights = []
    for values in (
        jnp.where(row_parts, -pltpu.roll(total_imag, OCTET, 1), total_real),
        jnp.where(row_parts, pltpu.roll(total_real, OCTET, 1), total_imag),
    ):
        values = jnp.where(lane_row < pair, values * scale, 0.0)
        width = pair
        while width < LANES:
            values = values + pltpu.roll(values, width, 1)
            width *= 2
        values = pltpu.roll(values, LANES - 2 * OCTET * mine, 1)
        weights.append(jnp.broadcast_to(values, (OCTET, LANES)))
    weights = jnp.concatenate(weights, 0)
    phase_id = lax.broadcasted_iota(jnp.int32, weights.shape, 0) % OCTET
    weight_lane = lax.broadcasted_iota(jnp.int32, weights.shape, 1)
    spans = [
        jnp.where((weight_lane + left) // pair == phase_id, weights, 0.0) for left in range(0, OCTET * pair, LANES)
    ]
    weights = jnp.concatenate(spans, 1)
    high = weights.astype(BF16)
    low = (weights - high.astype(F32)).astype(BF16)
    weights = jnp.concatenate([high, low], 0)
    weights_out[...] = weights
    pltpu.make_async_copy(sent, sent, send_sem2).wait()


def image_kernel(parts, weights, correction_in, focused, correction, image, own, sem):
    own[...] = correction_in[...]
    copies = [pltpu.make_async_copy(own, correction, sem.at[0])]
    copies[0].start()
    step = 2 * LANES
    columns = parts.shape[1]
    chunks = 4
    for c in range(chunks):
        begin, end = c * columns // chunks, (c + 1) * columns // chunks
        for left in range(begin, end, step):
            both = dot(weights[...], parts[:, left : left + step])
            both = both[0 : 2 * OCTET] + both[2 * OCTET :]
            for i in range(step // LANES):
                top = (left // LANES + i) * OCTET
                for h in range(2):
                    image[h, 0, top : top + OCTET, :] = both[h * OCTET : (h + 1) * OCTET, i * LANES : (i + 1) * LANES]
        span = pl.ds(begin // LANES * OCTET, (end - begin) // LANES * OCTET)
        copy = pltpu.make_async_copy(image.at[:, :, span], focused.at[:, :, span], sem.at[c + 1])
        copy.start()
        copies.append(copy)
    for copy in copies:
        copy.wait()


def solution(mesh):
    n = mesh.shape["tile"]

    def per_device(echoes, bin_start, bin_fraction, row_phase, column_phase, row_bin, column_bin):
        samples = echoes.shape[2]
        rows, columns = row_phase.shape[2], column_phase.shape[2]
        first, turn, last = tables(samples)
        bins = samples // LANES
        echo = echoes.reshape(2, bins, LANES)
        vmem = pl.BlockSpec(memory_space=pltpu.VMEM)
        operands = (
            bin_start, echo, jnp.asarray(first), jnp.asarray(turn), jnp.asarray(last),
            row_phase, column_phase, row_bin, column_bin, bin_fraction.T,
        )
        depth = n * 2 * n // LANES
        parts, weights, correction = pl.pallas_call(
            functools.partial(kernel, n),
            out_shape=(
                pltpu.VMEM((OCTET * 2 * n, rows // OCTET * columns), BF16),
                pltpu.VMEM((4 * OCTET, OCTET * 2 * n), BF16),
                pltpu.VMEM((1, 2), F32),
            ),
            in_specs=[pl.BlockSpec(memory_space=pltpu.HBM)] * len(operands),
            out_specs=(vmem, vmem, vmem),
            scratch_shapes=[pltpu.SMEM(bin_start.shape, jnp.int32)]
            + [pltpu.VMEM(operand.shape, operand.dtype) for operand in operands[1:9]]
            + [pltpu.SMEM((1, n), F32), pltpu.SemaphoreType.DMA((len(operands),))]
            + [
                pltpu.VMEM((2, bins + OCTET, LANES), F32),
                pltpu.VMEM((n, 4, LANES), BF16),
                pltpu.VMEM((n, 4, LANES), BF16),
                pltpu.VMEM((6, n // OCTET, OCTET, LANES), F32),
                pltpu.VMEM((n // OCTET, OCTET, LANES), F32),
                pltpu.VMEM((2, n // OCTET, rows, OCTET, LANES), jnp.int32),
                pltpu.VMEM((2, n // OCTET, rows, OCTET, LANES), F32),
                pltpu.VMEM((n // OCTET, 4 * OCTET, LANES), F32),
                pltpu.VMEM((n // OCTET, OCTET, LANES), F32),
                pltpu.VMEM((depth, LANES), F32),
                pltpu.VMEM((n, depth, LANES), F32),
                pltpu.SemaphoreType.DMA(()),
                pltpu.SemaphoreType.DMA((n // OCTET,)),
                pltpu.SemaphoreType.DMA(()),
                pltpu.SemaphoreType.DMA(()),
            ],
            compiler_params=pltpu.CompilerParams(collective_id=0, has_side_effects=True),
        )(*operands)
        hbm = pl.BlockSpec(memory_space=pltpu.HBM)
        focused, correction = pl.pallas_call(
            image_kernel,
            out_shape=(
                jax.ShapeDtypeStruct((2, 1, rows, columns), F32),
                jax.ShapeDtypeStruct((1, 2), F32),
            ),
            in_specs=[vmem] * 3,
            out_specs=(hbm, hbm),
            scratch_shapes=[
                pltpu.VMEM((2, 1, rows, columns), F32),
                pltpu.VMEM((1, 2), F32),
                pltpu.SemaphoreType.DMA((5,)),
            ],
        )(*[pltpu.with_memory_space_constraint(x, pltpu.VMEM) for x in (parts, weights, correction)])
        return focused, correction.T

    split = ("groups", "tile")
    in_specs = (
        P(None, split, None),
        P(split, None),
        P(None, split),
        P(None, split, None),
        P(None, split, None),
        P(None, split, None),
        P(None, split, None),
    )
    out_specs = (P(None, split, None, None), P(None, split))
    return jax.shard_map(per_device, mesh=mesh, in_specs=in_specs, out_specs=out_specs, check_vma=False)
```

```python
import functools
import math

import jax
import jax.numpy as jnp
import numpy as np
from jax import lax
from jax.experimental import pallas as pl
from jax.experimental.pallas import tpu as pltpu
from jax.sharding import PartitionSpec as P

LANES = 128
OCTET = 8
MESH = pl.DeviceIdType.MESH
F32 = jnp.float32
BF16 = jnp.bfloat16


def tables(samples):
    inner = LANES
    outer = samples // inner

    def wave(rows, columns, period):
        product = np.arange(rows)[:, None] * np.arange(columns)[None, :] % period
        phases = product * (2.0 * np.pi / period)
        return np.cos(phases), np.sin(phases)

    def split(table):
        table = table.astype(np.float32)
        high = table.astype(jnp.bfloat16)
        low = (table - high.astype(np.float32)).astype(jnp.bfloat16)
        return np.stack([high, low])

    first = split(np.concatenate(wave(outer, outer, outer), 1))
    last = split(np.concatenate(wave(inner, inner, inner), 1))
    turn = np.stack(wave(outer, inner, samples)) / math.sqrt(samples)
    return first, turn.astype(np.float32), last


def dot(a, b, dims=((1,), (0,)), precision=None):
    return lax.dot_general(a, b, (dims, ((), ())), precision=precision, preferred_element_type=F32)


def split3(table_ref, data, dims):
    high = data.astype(BF16)
    low = (data - high.astype(F32)).astype(BF16)
    return dot(table_ref[0], high, dims) + (dot(table_ref[1], high, dims) + dot(table_ref[0], low, dims))


def normalize(real_part, imag_part, axis, count):
    magnitude = real_part * real_part + imag_part * imag_part
    mean = jnp.sum(magnitude, axis=axis, keepdims=True) / count
    inverse = lax.rsqrt(magnitude + mean + 1e-06)
    return real_part * inverse, imag_part * inverse


def pick(source, index):
    numbers = lax.GatherDimensionNumbers(
        offset_dims=(), collapsed_slice_dims=(1,), start_index_map=(1,),
        operand_batching_dims=(0,), start_indices_batching_dims=(0,),
    )
    return lax.gather(
        source, index[..., None], numbers, (1, 1), mode=lax.GatherScatterMode.PROMISE_IN_BOUNDS
    )


def kernel(
    n, starts_in, echo_in, first_in, turn_in, last_in, row_phase_in, column_phase_in, row_bin_in, column_bin_in,
    fraction_in,
    parts, weights_out, correction,
    starts, echo, first, turn, last, row_phase, column_phase, row_bin, column_bin, fraction, in_sem,
    spec, outgoing, gathered, waves, share, index_all, steer, windows,
    message, messages,
    send_sem, recv_sem, send_sem2, recv_sem2,
):
    me = lax.axis_index("tile")
    rows = row_phase.shape[2]
    scale = 1.0 / math.sqrt(n)
    groups = n // OCTET
    mine = me // OCTET
    pair = 2 * n

    def group_of(slot):
        return lax.rem(mine + slot, groups)

    barrier = pltpu.get_barrier_semaphore()
    for k in range(1, n):
        pl.semaphore_signal(barrier, inc=1, device_id={"tile": lax.rem(me + k, n)}, device_id_type=MESH)

    sources = (
        starts_in, echo_in, first_in, turn_in, last_in, row_phase_in, column_phase_in, row_bin_in, column_bin_in,
        fraction_in,
    )
    targets = (starts, echo, first, turn, last, row_phase, column_phase, row_bin, column_bin, fraction)
    loads = [
        pltpu.make_async_copy(source, target, in_sem.at[i])
        for i, (source, target) in enumerate(zip(sources, targets))
    ]
    for load in loads[1:] + loads[:1]:
        load.start()

    upper = (2 * me) // n

    def other(k):
        place = upper * k + (1 - upper) * (n - 2 - k)
        return place + (place >= me).astype(jnp.int32)


    loads[1].wait()
    loads[2].wait()
    real, imag = echo[0], echo[1]
    data = jnp.concatenate(
        [jnp.concatenate([real, imag], 1), jnp.concatenate([imag, -real], 1)], 0
    )
    section = split3(first, data, ((1,), (0,)))
    half = section.shape[1] // 2
    loads[3].wait()
    loads[4].wait()
    real, imag = section[:, :half], section[:, half:]
    turned_real = real * turn[0] + imag * turn[1]
    turned_imag = imag * turn[0] - real * turn[1]
    data = jnp.concatenate(
        [jnp.concatenate([turned_real, turned_imag], 1), jnp.concatenate([turned_imag, -turned_real], 1)], 0
    )
    spectrum = split3(last, data, ((1,), (1,)))
    bins = spectrum.shape[0]
    spectrum = spectrum.astype(BF16).astype(F32)
    for h in range(2):
        spec[h, 0:bins, :] = spectrum[:, h * LANES : (h + 1) * LANES]
        spec[h, bins:, :] = jnp.zeros((spec.shape[1] - bins, LANES), F32)

    lane = lax.broadcasted_iota(jnp.int32, (OCTET, LANES), 1)
    loads[0].wait()
    for t in range(n):
        start = starts[0, t]
        top = start // LANES
        left = LANES - start % LANES
        pieces = []
        for h in range(2):
            moved = pltpu.roll(spec[h, pl.ds(top, OCTET), :], left % LANES, 1)
            below = pltpu.roll(moved, OCTET - 1, 0)
            pieces.append(jnp.where(lane < left, moved, below)[0:2])
        outgoing[t] = jnp.concatenate(pieces, 0).astype(BF16)

    pl.semaphore_wait(barrier, n - 1)

    def window_copy(device, slot):
        return pltpu.make_async_remote_copy(
            src_ref=outgoing.at[device],
            dst_ref=gathered.at[slot],
            send_sem=send_sem,
            recv_sem=recv_sem.at[slot // OCTET],
            device_id={"tile": device},
            device_id_type=MESH,
        )

    for k in range(n - 1):
        window_copy(other(k), me).start()
    pltpu.make_async_copy(outgoing.at[me], gathered.at[me], recv_sem.at[mine]).start()

    def rounded(values):
        return values.astype(BF16).astype(F32)

    for load in loads[5:]:
        load.wait()

    def by_octets(values):
        return values.reshape(groups, OCTET, LANES)

    row_angles, column_angles = row_phase[:, 0, :], column_phase[:, 0, :]
    for q, values in enumerate((
        jnp.cos(row_angles), jnp.sin(row_angles), jnp.cos(column_angles), jnp.sin(column_angles),
        row_bin[:, 0, :].astype(F32), column_bin[:, 0, :].astype(F32),
    )):
        waves[q] = by_octets(values)
    octet_id = lax.broadcasted_iota(jnp.int32, (OCTET, LANES), 0)
    tiles = rows // OCTET

    def spread(values, u):
        return jnp.broadcast_to(values[:, u : u + 1], (OCTET, LANES))

    tables = []
    for group in range(groups):
        part = jnp.zeros((OCTET, LANES), F32)
        for i in range(OCTET):
            part = jnp.where(octet_id == i, fraction[0, group * OCTET + i], part)
        share[group] = part
        tables.append([rounded(waves[q, group]) for q in range(6)])
    column_bin_of = [table[5].astype(jnp.int32) for table in tables]
    for u in range(rows):
        turns = [(spread(table[0], u), spread(table[1], u)) for table in tables]
        offsets = [spread(table[4], u) for table in tables]
        for slot, ((cosine, sine), offset, table) in enumerate(zip(turns, offsets, tables)):
            column_cosine, column_sine = table[2], table[3]
            offset = offset.astype(jnp.int32)
            index_all[0, slot, u] = (offset + column_bin_of[slot]) & (LANES - 1)
            index_all[1, slot, u] = offset
            steer[0, slot, u] = cosine * column_cosine - sine * column_sine
            steer[1, slot, u] = cosine * column_sine + sine * column_cosine

    def profiles(group):
        for i in range(OCTET):
            windows[group, 4 * i : 4 * (i + 1), :] = gathered[group * OCTET + i].astype(F32)
        window = [windows[group, pl.ds(q, OCTET, stride=4), :] for q in range(4)]
        moved = [pltpu.roll(values, LANES - 1, 1) for values in window]
        fraction_of = share[group]
        profile = []
        for q in range(4):
            shifted = moved[q] if q % 2 else jnp.where(lane == LANES - 1, moved[q + 1], moved[q])
            profile.append(rounded((1.0 - fraction_of) * window[q] + fraction_of * shifted))
        return profile

    def contribute(group, profile, u):
        low = index_all[0, group, u]
        is_low = index_all[1, group, u] <= lane
        real = pick(jnp.where(is_low, profile[0], profile[1]), low)
        imag = pick(jnp.where(is_low, profile[2], profile[3]), low)
        turn_real, turn_imag = steer[0, group, u], steer[1, group, u]
        both = jnp.concatenate([turn_real * real - turn_imag * imag, turn_real * imag + turn_imag * real], 0)
        top = pl.multiple_of((u % OCTET) * pair + group * 2 * OCTET, 2 * OCTET)
        left = (u // OCTET) * LANES
        parts[pl.ds(top, 2 * OCTET), left : left + LANES] = both.astype(BF16)

    def arrive(slot):
        group = group_of(slot)
        arrived = gathered.at[pl.ds(group * OCTET, OCTET)]
        pltpu.make_async_copy(arrived, arrived, recv_sem.at[group]).wait()
        return group, profiles(group)

    def visit(slot, carry):
        group, profile = arrive(slot)
        for u in range(rows):
            contribute(group, profile, u)
        return carry

    lax.fori_loop(0, groups - 1, visit, 0)
    group, profile = arrive(groups - 1)
    gram = jnp.zeros((pair, pair), F32)
    for a in range(OCTET):
        for u in range(a, rows, OCTET):
            contribute(group, profile, u)
        values = parts[a * pair : (a + 1) * pair, :]
        gram = gram + dot(values, values, ((1,), (1,)))
    gram = jnp.concatenate([gram, jnp.zeros((pair, LANES - pair), F32)], 1)
    imag_lane = (lane // OCTET) % 2 == 1
    folds = LANES // pair
    packed = []
    for g in range(groups):
        top = g * 2 * OCTET
        real, imag = gram[top : top + OCTET], gram[top + OCTET : top + 2 * OCTET]
        values = real + jnp.where(
            imag_lane, -pltpu.roll(imag, OCTET, 1), pltpu.roll(imag, LANES - OCTET, 1)
        )
        values = jnp.where(lane < pair, values, 0.0)
        if g % folds == 0:
            packed.append(values)
        else:
            packed[-1] = packed[-1] + pltpu.roll(values, g % folds * pair, 1)
    packed = jnp.concatenate(packed, 0)
    message[...] = packed
    messages[me] = packed

    def gram_copy(device, slot):
        return pltpu.make_async_remote_copy(
            src_ref=message,
            dst_ref=messages.at[slot],
            send_sem=send_sem2,
            recv_sem=recv_sem2,
            device_id={"tile": device},
            device_id_type=MESH,
        )

    for k in range(n - 1):
        gram_copy(other(k), me).start()
    sent = outgoing.at[pl.ds(0, n - 1)]
    pltpu.make_async_copy(sent, sent, send_sem).wait()
    sent = messages.at[pl.ds(0, n - 1)]
    pltpu.make_async_copy(sent, sent, recv_sem2).wait()

    total = jnp.sum(messages[...], axis=0)
    gram = []
    for g in range(groups):
        top = g // folds * OCTET
        values = total[top : top + OCTET]
        gram.append(values if g % folds == 0 else pltpu.roll(values, LANES - g % folds * pair, 1))
    gram = jnp.concatenate(gram, 0)
    row_id = lax.broadcasted_iota(jnp.int32, gram.shape, 0)
    lane_id = lax.broadcasted_iota(jnp.int32, gram.shape, 1)
    column_id = lane_id // (2 * OCTET) * OCTET + lane_id % OCTET
    off_diagonal = (lane_id < pair) & (lane_id // OCTET % 2 == 0) & (column_id != row_id)
    gram_real = jnp.where(off_diagonal, gram * scale, 0.0)
    gram_imag = jnp.where(off_diagonal, pltpu.roll(gram, LANES - OCTET, 1) * scale, 0.0)

    def along(values, axis):
        return jnp.sum(values, axis=axis, keepdims=True)

    one_real, one_imag = normalize(along(gram_real, 1), along(gram_imag, 1), 0, n)
    row_real, row_imag = normalize(along(gram_real, 0), -along(gram_imag, 0), 1, n)
    rest_real = along(gram_real * one_real + gram_imag * one_imag, 0)
    rest_imag = along(gram_real * one_imag - gram_imag * one_real, 0)
    again_real = row_real * rest_real + row_imag * rest_imag
    again_imag = row_real * rest_imag - row_imag * rest_real
    two_real, two_imag = normalize(again_real, again_imag, 1, n)
    total_real = row_real * two_real - row_imag * two_imag
    total_imag = row_real * two_imag + row_imag * two_real
    lane_row = lax.broadcasted_iota(jnp.int32, total_real.shape, 1)
    own_lane = (me // OCTET) * 2 * OCTET + me % OCTET
    own = lane_row == own_lane
    correction[...] = jnp.concatenate(
        [along(jnp.where(own, total_real, 0.0), 1), along(jnp.where(own, total_imag, 0.0), 1)], 1
    )
    row_parts = (lane_row // OCTET) % 2 == 1
    weights = []
    for values in (
        jnp.where(row_parts, -pltpu.roll(total_imag, OCTET, 1), total_real),
        jnp.where(row_parts, pltpu.roll(total_real, OCTET, 1), total_imag),
    ):
        values = jnp.where(lane_row < pair, values * scale, 0.0)
        width = pair
        while width < LANES:
            values = values + pltpu.roll(values, width, 1)
            width *= 2
        weights.append(jnp.broadcast_to(values, (OCTET, LANES)))
    weights = jnp.concatenate(weights, 0)
    phase_id = lax.broadcasted_iota(jnp.int32, weights.shape, 0) % OCTET
    weight_lane = lax.broadcasted_iota(jnp.int32, weights.shape, 1)
    spans = [
        jnp.where((weight_lane + left) // pair == phase_id, weights, 0.0) for left in range(0, OCTET * pair, LANES)
    ]
    weights = jnp.concatenate(spans, 1)
    high = weights.astype(BF16)
    low = (weights - high.astype(F32)).astype(BF16)
    weights = jnp.concatenate([high, low], 0)
    weights_out[...] = weights
    pltpu.make_async_copy(sent, sent, send_sem2).wait()


def image_kernel(parts, weights, correction_in, focused, correction, image, own, sem):
    own[...] = correction_in[...]
    copies = [pltpu.make_async_copy(own, correction, sem.at[0])]
    copies[0].start()
    step = 2 * LANES
    columns = parts.shape[1]
    chunks = 4
    for c in range(chunks):
        begin, end = c * columns // chunks, (c + 1) * columns // chunks
        for left in range(begin, end, step):
            both = dot(weights[...], parts[:, left : left + step])
            both = both[0 : 2 * OCTET] + both[2 * OCTET :]
            for i in range(step // LANES):
                top = (left // LANES + i) * OCTET
                for h in range(2):
                    image[h, 0, top : top + OCTET, :] = both[h * OCTET : (h + 1) * OCTET, i * LANES : (i + 1) * LANES]
        span = pl.ds(begin // LANES * OCTET, (end - begin) // LANES * OCTET)
        copy = pltpu.make_async_copy(image.at[:, :, span], focused.at[:, :, span], sem.at[c + 1])
        copy.start()
        copies.append(copy)
    for copy in copies:
        copy.wait()


def solution(mesh):
    n = mesh.shape["tile"]

    def per_device(echoes, bin_start, bin_fraction, row_phase, column_phase, row_bin, column_bin):
        samples = echoes.shape[2]
        rows, columns = row_phase.shape[2], column_phase.shape[2]
        first, turn, last = tables(samples)
        bins = samples // LANES
        echo = echoes.reshape(2, bins, LANES)
        vmem = pl.BlockSpec(memory_space=pltpu.VMEM)
        operands = (
            bin_start, echo, jnp.asarray(first), jnp.asarray(turn), jnp.asarray(last),
            row_phase, column_phase, row_bin, column_bin, bin_fraction.T,
        )
        depth = -(-n * 2 * n // (OCTET * LANES)) * OCTET
        parts, weights, correction = pl.pallas_call(
            functools.partial(kernel, n),
            out_shape=(
                pltpu.VMEM((OCTET * 2 * n, rows // OCTET * columns), BF16),
                pltpu.VMEM((4 * OCTET, OCTET * 2 * n), BF16),
                pltpu.VMEM((1, 2), F32),
            ),
            in_specs=[pl.BlockSpec(memory_space=pltpu.HBM)] * len(operands),
            out_specs=(vmem, vmem, vmem),
            scratch_shapes=[pltpu.SMEM(bin_start.shape, jnp.int32)]
            + [pltpu.VMEM(operand.shape, operand.dtype) for operand in operands[1:9]]
            + [pltpu.SMEM((1, n), F32), pltpu.SemaphoreType.DMA((len(operands),))]
            + [
                pltpu.VMEM((2, bins + OCTET, LANES), F32),
                pltpu.VMEM((n, 4, LANES), BF16),
                pltpu.VMEM((n, 4, LANES), BF16),
                pltpu.VMEM((6, n // OCTET, OCTET, LANES), F32),
                pltpu.VMEM((n // OCTET, OCTET, LANES), F32),
                pltpu.VMEM((2, n // OCTET, rows, OCTET, LANES), jnp.int32),
                pltpu.VMEM((2, n // OCTET, rows, OCTET, LANES), F32),
                pltpu.VMEM((n // OCTET, 4 * OCTET, LANES), F32),
                pltpu.VMEM((depth, LANES), F32),
                pltpu.VMEM((n, depth, LANES), F32),
                pltpu.SemaphoreType.DMA(()),
                pltpu.SemaphoreType.DMA((n // OCTET,)),
                pltpu.SemaphoreType.DMA(()),
                pltpu.SemaphoreType.DMA(()),
            ],
            compiler_params=pltpu.CompilerParams(collective_id=0, has_side_effects=True),
        )(*operands)
        hbm = pl.BlockSpec(memory_space=pltpu.HBM)
        focused, correction = pl.pallas_call(
            image_kernel,
            out_shape=(
                jax.ShapeDtypeStruct((2, 1, rows, columns), F32),
                jax.ShapeDtypeStruct((1, 2), F32),
            ),
            in_specs=[vmem] * 3,
            out_specs=(hbm, hbm),
            scratch_shapes=[
                pltpu.VMEM((2, 1, rows, columns), F32),
                pltpu.VMEM((1, 2), F32),
                pltpu.SemaphoreType.DMA((5,)),
            ],
        )(*[pltpu.with_memory_space_constraint(x, pltpu.VMEM) for x in (parts, weights, correction)])
        return focused, correction.T

    split = ("groups", "tile")
    in_specs = (
        P(None, split, None),
        P(split, None),
        P(None, split),
        P(None, split, None),
        P(None, split, None),
        P(None, split, None),
        P(None, split, None),
    )
    out_specs = (P(None, split, None, None), P(None, split))
    return jax.shard_map(per_device, mesh=mesh, in_specs=in_specs, out_specs=out_specs, check_vma=False)
```

```python
import functools
import math

import jax
import jax.numpy as jnp
import numpy as np
from jax import lax
from jax.experimental import pallas as pl
from jax.experimental.pallas import tpu as pltpu
from jax.sharding import PartitionSpec as P

LANES = 128
OCTET = 8
QUAD = 4
MESH = pl.DeviceIdType.MESH
F32 = jnp.float32
BF16 = jnp.bfloat16


def tables(samples):
    inner = LANES
    outer = samples // inner

    def wave(rows, columns, period):
        product = np.arange(rows)[:, None] * np.arange(columns)[None, :] % period
        phases = product * (2.0 * np.pi / period)
        return np.cos(phases), np.sin(phases)

    def split(table):
        table = table.astype(np.float32)
        high = table.astype(jnp.bfloat16)
        low = (table - high.astype(np.float32)).astype(jnp.bfloat16)
        return np.stack([high, low])

    first = split(np.concatenate(wave(outer, outer, outer), 1))
    last = split(np.concatenate(wave(inner, inner, inner), 1))
    turn = np.stack(wave(outer, inner, samples)) / math.sqrt(samples)
    return first, turn.astype(np.float32), last


def dot(a, b, dims=((1,), (0,)), precision=None):
    return lax.dot_general(a, b, (dims, ((), ())), precision=precision, preferred_element_type=F32)


def split3(table_ref, data, dims):
    high = data.astype(BF16)
    low = (data - high.astype(F32)).astype(BF16)
    return dot(table_ref[0], high, dims) + (dot(table_ref[1], high, dims) + dot(table_ref[0], low, dims))


def normalize(real_part, imag_part, axis, count):
    magnitude = real_part * real_part + imag_part * imag_part
    mean = jnp.sum(magnitude, axis=axis, keepdims=True) / count
    inverse = lax.rsqrt(magnitude + mean + 1e-06)
    return real_part * inverse, imag_part * inverse


def pick(source, index):
    numbers = lax.GatherDimensionNumbers(
        offset_dims=(), collapsed_slice_dims=(1,), start_index_map=(1,),
        operand_batching_dims=(0,), start_indices_batching_dims=(0,),
    )
    return lax.gather(
        source, index[..., None], numbers, (1, 1), mode=lax.GatherScatterMode.PROMISE_IN_BOUNDS
    )


def kernel(
    n, starts_in, echo_in, first_in, turn_in, last_in, row_phase_in, column_phase_in, row_bin_in, column_bin_in,
    fraction_in,
    parts, weights_out, correction,
    starts, echo, first, turn, last, row_phase, column_phase, row_bin, column_bin, fraction, in_sem,
    spec, outgoing, gathered, waves, share, index_all, steer, windows,
    message, messages,
    send_sem, recv_sem, send_sem2, recv_sem2,
):
    me = lax.axis_index("tile")
    rows = row_phase.shape[2]
    scale = 1.0 / math.sqrt(n)
    groups = n // QUAD
    mine = me // QUAD
    pair = 2 * n

    barrier = pltpu.get_barrier_semaphore()
    for k in range(1, n):
        pl.semaphore_signal(barrier, inc=1, device_id={"tile": lax.rem(me + k, n)}, device_id_type=MESH)

    sources = (
        starts_in, echo_in, first_in, turn_in, last_in, row_phase_in, column_phase_in, row_bin_in, column_bin_in,
        fraction_in,
    )
    targets = (starts, echo, first, turn, last, row_phase, column_phase, row_bin, column_bin, fraction)
    loads = [
        pltpu.make_async_copy(source, target, in_sem.at[i])
        for i, (source, target) in enumerate(zip(sources, targets))
    ]
    for load in loads[1:] + loads[:1]:
        load.start()

    upper = (2 * me) // n

    def group_of(slot):
        place = upper * (groups - 1 - slot) + (1 - upper) * (slot - 1)
        place = place + (place >= mine).astype(jnp.int32)
        return place if isinstance(slot, int) else jnp.where(slot == 0, mine, place)

    def other(k):
        place = upper * k + (1 - upper) * (n - 2 - k)
        return place + (place >= me).astype(jnp.int32)


    loads[1].wait()
    loads[2].wait()
    real, imag = echo[0], echo[1]
    data = jnp.concatenate(
        [jnp.concatenate([real, imag], 1), jnp.concatenate([imag, -real], 1)], 0
    )
    section = split3(first, data, ((1,), (0,)))
    half = section.shape[1] // 2
    loads[3].wait()
    loads[4].wait()
    real, imag = section[:, :half], section[:, half:]
    turned_real = real * turn[0] + imag * turn[1]
    turned_imag = imag * turn[0] - real * turn[1]
    data = jnp.concatenate(
        [jnp.concatenate([turned_real, turned_imag], 1), jnp.concatenate([turned_imag, -turned_real], 1)], 0
    )
    spectrum = split3(last, data, ((1,), (1,)))
    bins = spectrum.shape[0]
    spectrum = spectrum.astype(BF16).astype(F32)
    for h in range(2):
        spec[h, 0:bins, :] = spectrum[:, h * LANES : (h + 1) * LANES]
        spec[h, bins:, :] = jnp.zeros((spec.shape[1] - bins, LANES), F32)

    lane = lax.broadcasted_iota(jnp.int32, (OCTET, LANES), 1)
    loads[0].wait()
    for t in range(n):
        start = starts[0, t]
        top = start // LANES
        left = LANES - start % LANES
        pieces = []
        for h in range(2):
            moved = pltpu.roll(spec[h, pl.ds(top, OCTET), :], left % LANES, 1)
            below = pltpu.roll(moved, OCTET - 1, 0)
            pieces.append(jnp.where(lane < left, moved, below)[0:2])
        outgoing[t] = jnp.concatenate(pieces, 0).astype(BF16)

    pl.semaphore_wait(barrier, n - 1)

    def window_copy(device, slot):
        return pltpu.make_async_remote_copy(
            src_ref=outgoing.at[device],
            dst_ref=gathered.at[slot],
            send_sem=send_sem,
            recv_sem=recv_sem.at[slot // QUAD],
            device_id={"tile": device},
            device_id_type=MESH,
        )

    for k in range(n - 1):
        window_copy(other(k), me).start()
    pltpu.make_async_copy(outgoing.at[me], gathered.at[me], recv_sem.at[mine]).start()

    def rounded(values):
        return values.astype(BF16).astype(F32)

    for load in loads[5:]:
        load.wait()

    row_angles, column_angles = row_phase[:, 0, :], column_phase[:, 0, :]
    for q, values in enumerate((
        jnp.cos(row_angles), jnp.sin(row_angles), jnp.cos(column_angles), jnp.sin(column_angles),
        row_bin[:, 0, :].astype(F32), column_bin[:, 0, :].astype(F32),
    )):
        values = values.reshape(groups, QUAD, LANES)
        waves[q, :, 0:QUAD] = values
        waves[q, :, QUAD:] = values
    octet_id = lax.broadcasted_iota(jnp.int32, (OCTET, LANES), 0)
    tiles = rows // OCTET

    pairs = [(a, t) for a in range(OCTET) for t in range(0, tiles, 2)]
    upper_half = octet_id >= QUAD
    second_row = jnp.where(upper_half, OCTET, 0)

    def spread(values, pattern):
        return pick(values, pattern)

    tables = []
    for group in range(groups):
        part = jnp.zeros((OCTET, LANES), F32)
        for i in range(QUAD):
            part = jnp.where(octet_id & (QUAD - 1) == i, fraction[0, group * QUAD + i], part)
        share[group] = part
        tables.append([rounded(waves[q, group]) for q in range(6)])
    column_bin_of = [table[5].astype(jnp.int32) for table in tables]
    for u, (a, t) in enumerate(pairs):
        pattern = second_row + (t * OCTET + a)
        turns = [(spread(table[0], pattern), spread(table[1], pattern)) for table in tables]
        offsets = [spread(table[4], pattern) for table in tables]
        for slot, ((cosine, sine), offset, table) in enumerate(zip(turns, offsets, tables)):
            column_cosine, column_sine = table[2], table[3]
            offset = offset.astype(jnp.int32)
            index_all[0, slot, u] = (offset + column_bin_of[slot]) & (LANES - 1)
            index_all[1, slot, u] = offset
            steer[0, slot, u] = cosine * column_cosine - sine * column_sine
            steer[1, slot, u] = cosine * column_sine + sine * column_cosine

    def profiles(group):
        for i in range(QUAD):
            values = gathered[group * QUAD + i].astype(F32)
            for j in (i, i + QUAD):
                windows[group, 4 * j : 4 * (j + 1), :] = values
        window = [windows[group, pl.ds(q, OCTET, stride=4), :] for q in range(4)]
        moved = [pltpu.roll(values, LANES - 1, 1) for values in window]
        fraction_of = share[group]
        profile = []
        for q in range(4):
            shifted = moved[q] if q % 2 else jnp.where(lane == LANES - 1, moved[q + 1], moved[q])
            profile.append(rounded((1.0 - fraction_of) * window[q] + fraction_of * shifted))
        return profile

    def contribute(group, profile, u):
        low = index_all[0, group, u]
        is_low = index_all[1, group, u] <= lane
        real = pick(jnp.where(is_low, profile[0], profile[1]), low)
        imag = pick(jnp.where(is_low, profile[2], profile[3]), low)
        turn_real, turn_imag = steer[0, group, u], steer[1, group, u]
        part_real = turn_real * real - turn_imag * imag
        part_imag = turn_real * imag + turn_imag * real
        a, t = pairs[u]
        top = pl.multiple_of(a * pair + group * OCTET, OCTET)
        both = (
            jnp.where(upper_half, pltpu.roll(part_imag, QUAD, 0), part_real),
            jnp.where(upper_half, part_imag, pltpu.roll(part_real, QUAD, 0)),
        )
        for h in range(2):
            left = (t + h) * LANES
            parts[pl.ds(top, OCTET), left : left + LANES] = both[h].astype(BF16)

    def arrive(slot):
        group = group_of(slot)
        arrived = gathered.at[pl.ds(group * QUAD, QUAD)]
        pltpu.make_async_copy(arrived, arrived, recv_sem.at[group]).wait()
        return group, profiles(group)

    def visit(slot, carry):
        group, profile = arrive(slot)
        for u in range(len(pairs)):
            contribute(group, profile, u)
        return carry

    lax.fori_loop(0, groups - 1, visit, 0)
    group, profile = arrive(groups - 1)
    grams = [jnp.zeros((pair, pair), F32)] * 2
    for a in range(OCTET):
        for u in range(a * tiles // 2, (a + 1) * tiles // 2):
            contribute(group, profile, u)
        half = tiles // 2 * LANES
        for h in range(2):
            values = parts[a * pair : (a + 1) * pair, h * half : (h + 1) * half]
            grams[h] = grams[h] + dot(values, values, ((1,), (1,)))
    gram = jnp.concatenate([grams[0] + grams[1], jnp.zeros((pair, LANES - pair), F32)], 1)
    folds = LANES // pair
    octets = n // OCTET

    def turned(values, shift):
        return pltpu.roll(values, shift % LANES, 1) if shift % LANES else values

    packed = [jnp.zeros((OCTET, LANES), F32)] * (-(-2 * octets // folds))
    for g in range(octets):
        first = gram[2 * g * OCTET : (2 * g + 1) * OCTET]
        second = gram[(2 * g + 1) * OCTET : (2 * g + 2) * OCTET]
        real = jnp.where(upper_half, pltpu.roll(second, QUAD, 0), first)
        imag = jnp.where(upper_half, second, pltpu.roll(first, QUAD, 0))
        for place in (g, octets + g):
            left = place % folds * pair
            if place == g:
                values = turned(real, left) + turned(imag, left - QUAD)
            else:
                values = turned(real, left - QUAD) - turned(imag, left)
            packed[place // folds] = jnp.where(lane & -pair == left, values, packed[place // folds])
    packed = jnp.concatenate([jnp.where((lane & QUAD) == 0, values, 0.0) for values in packed], 0)
    message[...] = packed
    messages[me] = packed

    def gram_copy(device, slot):
        return pltpu.make_async_remote_copy(
            src_ref=message,
            dst_ref=messages.at[slot],
            send_sem=send_sem2,
            recv_sem=recv_sem2,
            device_id={"tile": device},
            device_id_type=MESH,
        )

    for k in range(n - 1):
        gram_copy(other(k), me).start()
    sent = outgoing.at[pl.ds(0, n - 1)]
    pltpu.make_async_copy(sent, sent, send_sem).wait()
    sent = messages.at[pl.ds(0, n - 1)]
    pltpu.make_async_copy(sent, sent, recv_sem2).wait()

    total = jnp.sum(messages[...], axis=0)
    gram = []
    for place in range(2 * octets):
        top = place // folds * OCTET
        gram.append(turned(total[top : top + OCTET], -(place % folds * pair)))
    gram, gram_imag = jnp.concatenate(gram[:octets], 0), jnp.concatenate(gram[octets:], 0)
    row_id = lax.broadcasted_iota(jnp.int32, gram.shape, 0)
    lane_id = lax.broadcasted_iota(jnp.int32, gram.shape, 1)
    column_id = ((lane_id >> 1) & -QUAD) + (lane_id & (QUAD - 1))
    off_diagonal = (lane_id < pair) & ((lane_id & QUAD) == 0) & (column_id != row_id)
    gram_real = jnp.where(off_diagonal, gram * scale, 0.0)
    gram_imag = jnp.where(off_diagonal, gram_imag * scale, 0.0)

    def along(values, axis):
        return jnp.sum(values, axis=axis, keepdims=True)

    one_real, one_imag = normalize(along(gram_real, 1), along(gram_imag, 1), 0, n)
    row_real, row_imag = normalize(along(gram_real, 0), -along(gram_imag, 0), 1, n)
    rest_real = along(gram_real * one_real + gram_imag * one_imag, 0)
    rest_imag = along(gram_real * one_imag - gram_imag * one_real, 0)
    again_real = row_real * rest_real + row_imag * rest_imag
    again_imag = row_real * rest_imag - row_imag * rest_real
    two_real, two_imag = normalize(again_real, again_imag, 1, n)
    total_real = row_real * two_real - row_imag * two_imag
    total_imag = row_real * two_imag + row_imag * two_real
    lane_row = lax.broadcasted_iota(jnp.int32, total_real.shape, 1)
    own_lane = mine * 2 * QUAD + me % QUAD
    own = lane_row == own_lane
    correction[...] = jnp.concatenate(
        [along(jnp.where(own, total_real, 0.0), 1), along(jnp.where(own, total_imag, 0.0), 1)], 1
    )
    weights = []
    for straight, crossed in ((total_real, -total_imag), (total_imag, total_real)):
        copies = []
        for left in range(0, LANES, pair):
            copies += [turned(straight * scale, left), turned(crossed * scale, left + QUAD)]
        while len(copies) > 1:
            copies = [x + y for x, y in zip(copies[::2], copies[1::2])]
        weights.append(jnp.broadcast_to(copies[0], (OCTET, LANES)))
    weights = jnp.concatenate(weights, 0)
    phase_id = lax.broadcasted_iota(jnp.int32, weights.shape, 0) & (OCTET - 1)
    weight_lane = lax.broadcasted_iota(jnp.int32, weights.shape, 1)
    spans = [
        jnp.where((weight_lane + left) & -pair == phase_id * pair, weights, 0.0) for left in range(0, OCTET * pair, LANES)
    ]
    weights = jnp.concatenate(spans, 1)
    high = weights.astype(BF16)
    low = (weights - high.astype(F32)).astype(BF16)
    weights = jnp.concatenate([high, low], 0)
    weights_out[...] = weights
    pltpu.make_async_copy(sent, sent, send_sem2).wait()


def image_kernel(parts, weights, correction_in, focused, correction, image, own, sem):
    own[...] = correction_in[...]
    copies = [pltpu.make_async_copy(own, correction, sem.at[0])]
    copies[0].start()
    step = 2 * LANES
    columns = parts.shape[1]
    chunks = 4
    for c in range(chunks):
        begin, end = c * columns // chunks, (c + 1) * columns // chunks
        for left in range(begin, end, step):
            both = dot(weights[...], parts[:, left : left + step])
            both = both[0 : 2 * OCTET] + both[2 * OCTET :]
            for i in range(step // LANES):
                top = (left // LANES + i) * OCTET
                for h in range(2):
                    image[h, 0, top : top + OCTET, :] = both[h * OCTET : (h + 1) * OCTET, i * LANES : (i + 1) * LANES]
        span = pl.ds(begin // LANES * OCTET, (end - begin) // LANES * OCTET)
        copy = pltpu.make_async_copy(image.at[:, :, span], focused.at[:, :, span], sem.at[c + 1])
        copy.start()
        copies.append(copy)
    for copy in copies:
        copy.wait()


def solution(mesh):
    n = mesh.shape["tile"]

    def per_device(echoes, bin_start, bin_fraction, row_phase, column_phase, row_bin, column_bin):
        samples = echoes.shape[2]
        rows, columns = row_phase.shape[2], column_phase.shape[2]
        first, turn, last = tables(samples)
        bins = samples // LANES
        echo = echoes.reshape(2, bins, LANES)
        vmem = pl.BlockSpec(memory_space=pltpu.VMEM)
        operands = (
            bin_start, echo, jnp.asarray(first), jnp.asarray(turn), jnp.asarray(last),
            row_phase, column_phase, row_bin, column_bin, bin_fraction.T,
        )
        depth = -(-4 * n * n // (OCTET * LANES)) * OCTET
        parts, weights, correction = pl.pallas_call(
            functools.partial(kernel, n),
            out_shape=(
                pltpu.VMEM((OCTET * 2 * n, rows // OCTET * columns), BF16),
                pltpu.VMEM((4 * OCTET, OCTET * 2 * n), BF16),
                pltpu.VMEM((1, 2), F32),
            ),
            in_specs=[pl.BlockSpec(memory_space=pltpu.HBM)] * len(operands),
            out_specs=(vmem, vmem, vmem),
            scratch_shapes=[pltpu.SMEM(bin_start.shape, jnp.int32)]
            + [pltpu.VMEM(operand.shape, operand.dtype) for operand in operands[1:9]]
            + [pltpu.SMEM((1, n), F32), pltpu.SemaphoreType.DMA((len(operands),))]
            + [
                pltpu.VMEM((2, bins + OCTET, LANES), F32),
                pltpu.VMEM((n, 4, LANES), BF16),
                pltpu.VMEM((n, 4, LANES), BF16),
                pltpu.VMEM((6, n // QUAD, OCTET, LANES), F32),
                pltpu.VMEM((n // QUAD, OCTET, LANES), F32),
                pltpu.VMEM((2, n // QUAD, rows // 2, OCTET, LANES), jnp.int32),
                pltpu.VMEM((2, n // QUAD, rows // 2, OCTET, LANES), F32),
                pltpu.VMEM((n // QUAD, 4 * OCTET, LANES), F32),
                pltpu.VMEM((depth, LANES), F32),
                pltpu.VMEM((n, depth, LANES), F32),
                pltpu.SemaphoreType.DMA(()),
                pltpu.SemaphoreType.DMA((n // QUAD,)),
                pltpu.SemaphoreType.DMA(()),
                pltpu.SemaphoreType.DMA(()),
            ],
            compiler_params=pltpu.CompilerParams(collective_id=0, has_side_effects=True),
        )(*operands)
        hbm = pl.BlockSpec(memory_space=pltpu.HBM)
        focused, correction = pl.pallas_call(
            image_kernel,
            out_shape=(
                jax.ShapeDtypeStruct((2, 1, rows, columns), F32),
                jax.ShapeDtypeStruct((1, 2), F32),
            ),
            in_specs=[vmem] * 3,
            out_specs=(hbm, hbm),
            scratch_shapes=[
                pltpu.VMEM((2, 1, rows, columns), F32),
                pltpu.VMEM((1, 2), F32),
                pltpu.SemaphoreType.DMA((5,)),
            ],
        )(*[pltpu.with_memory_space_constraint(x, pltpu.VMEM) for x in (parts, weights, correction)])
        return focused, correction.T

    split = ("groups", "tile")
    in_specs = (
        P(None, split, None),
        P(split, None),
        P(None, split),
        P(None, split, None),
        P(None, split, None),
        P(None, split, None),
        P(None, split, None),
    )
    out_specs = (P(None, split, None, None), P(None, split))
    return jax.shard_map(per_device, mesh=mesh, in_specs=in_specs, out_specs=out_specs, check_vma=False)
```

```python
import functools
import math

import jax
import jax.numpy as jnp
import numpy as np
from jax import lax
from jax.experimental import pallas as pl
from jax.experimental.pallas import tpu as pltpu
from jax.sharding import PartitionSpec as P

LANES = 128
OCTET = 8
QUAD = 4
MESH = pl.DeviceIdType.MESH
F32 = jnp.float32
BF16 = jnp.bfloat16


def tables(samples):
    inner = LANES
    outer = samples // inner

    def wave(rows, columns, period):
        product = np.arange(rows)[:, None] * np.arange(columns)[None, :] % period
        phases = product * (2.0 * np.pi / period)
        return np.cos(phases), np.sin(phases)

    def split(table):
        table = table.astype(np.float32)
        high = table.astype(jnp.bfloat16)
        low = (table - high.astype(np.float32)).astype(jnp.bfloat16)
        return np.stack([high, low])

    first = split(np.concatenate(wave(outer, outer, outer), 1))
    last = split(np.concatenate(wave(inner, inner, inner), 1))
    turn = np.stack(wave(outer, inner, samples)) / math.sqrt(samples)
    return first, turn.astype(np.float32), last


def dot(a, b, dims=((1,), (0,)), precision=None):
    return lax.dot_general(a, b, (dims, ((), ())), precision=precision, preferred_element_type=F32)


def split3(table_ref, data, dims):
    high = data.astype(BF16)
    low = (data - high.astype(F32)).astype(BF16)
    return dot(table_ref[0], high, dims) + (dot(table_ref[1], high, dims) + dot(table_ref[0], low, dims))


def normalize(real_part, imag_part, mean):
    inverse = lax.rsqrt(real_part * real_part + imag_part * imag_part + mean + 1e-06)
    return real_part * inverse, imag_part * inverse


def pick(source, index):
    numbers = lax.GatherDimensionNumbers(
        offset_dims=(), collapsed_slice_dims=(1,), start_index_map=(1,),
        operand_batching_dims=(0,), start_indices_batching_dims=(0,),
    )
    return lax.gather(
        source, index[..., None], numbers, (1, 1), mode=lax.GatherScatterMode.PROMISE_IN_BOUNDS
    )


def kernel(
    n, starts_in, echo_in, first_in, turn_in, last_in, row_phase_in, column_phase_in, row_bin_in, column_bin_in,
    fraction_in,
    parts, weights_out, correction,
    starts, echo, first, turn, last, row_phase, column_phase, row_bin, column_bin, fraction, in_sem,
    spec, outgoing, gathered, waves, share, index_all, steer, windows,
    message, messages,
    send_sem, recv_sem, send_sem2, recv_sem2,
):
    me = lax.axis_index("tile")
    rows = row_phase.shape[2]
    scale = 1.0 / math.sqrt(n)
    groups = n // QUAD
    mine = me // QUAD
    pair = 2 * n

    barrier = pltpu.get_barrier_semaphore()
    for k in range(1, n):
        pl.semaphore_signal(barrier, inc=1, device_id={"tile": lax.rem(me + k, n)}, device_id_type=MESH)

    sources = (
        starts_in, echo_in, first_in, turn_in, last_in, row_phase_in, column_phase_in, row_bin_in, column_bin_in,
        fraction_in,
    )
    targets = (starts, echo, first, turn, last, row_phase, column_phase, row_bin, column_bin, fraction)
    last_load = len(sources) - 1
    loads = [
        pltpu.make_async_copy(source, target, in_sem.at[0 if i == 0 else 1 if i == last_load else 2])
        for i, (source, target) in enumerate(zip(sources, targets))
    ]
    for load in loads[1:] + loads[:1]:
        load.start()

    upper = (2 * me) // n

    def group_of(slot):
        place = upper * (groups - 1 - slot) + (1 - upper) * (slot - 1)
        place = place + (place >= mine).astype(jnp.int32)
        return place if isinstance(slot, int) else jnp.where(slot == 0, mine, place)

    def other(k):
        place = upper * k + (1 - upper) * (n - 2 - k)
        return place + (place >= me).astype(jnp.int32)


    size = sum(math.prod(target.shape) * target.dtype.itemsize for target in targets[1:-1])
    loaded = parts.at[pl.ds(0, size // (2 * parts.shape[1]))]
    pltpu.make_async_copy(loaded, loaded, in_sem.at[2]).wait()
    real, imag = echo[0], echo[1]
    data = jnp.concatenate(
        [jnp.concatenate([real, imag], 1), jnp.concatenate([imag, -real], 1)], 0
    )
    section = split3(first, data, ((1,), (0,)))
    half = section.shape[1] // 2
    real, imag = section[:, :half], section[:, half:]
    turned_real = real * turn[0] + imag * turn[1]
    turned_imag = imag * turn[0] - real * turn[1]
    data = jnp.concatenate(
        [jnp.concatenate([turned_real, turned_imag], 1), jnp.concatenate([turned_imag, -turned_real], 1)], 0
    )
    spectrum = split3(last, data, ((1,), (1,)))
    bins = spectrum.shape[0]
    spectrum = spectrum.astype(BF16).astype(F32)
    for h in range(2):
        spec[h, 0:bins, :] = spectrum[:, h * LANES : (h + 1) * LANES]
        spec[h, bins:, :] = jnp.zeros((spec.shape[1] - bins, LANES), F32)

    lane = lax.broadcasted_iota(jnp.int32, (OCTET, LANES), 1)
    loads[0].wait()
    for t in range(n):
        start = starts[0, t]
        top = start // LANES
        left = LANES - start % LANES
        pieces = []
        for h in range(2):
            moved = pltpu.roll(spec[h, pl.ds(top, OCTET), :], left % LANES, 1)
            below = pltpu.roll(moved, OCTET - 1, 0)
            pieces.append(jnp.where(lane < left, moved, below)[0:2])
        outgoing[t] = jnp.concatenate(pieces, 0).astype(BF16)

    pl.semaphore_wait(barrier, n - 1)

    def window_copy(device, slot):
        return pltpu.make_async_remote_copy(
            src_ref=outgoing.at[device],
            dst_ref=gathered.at[slot],
            send_sem=send_sem,
            recv_sem=recv_sem.at[slot // QUAD],
            device_id={"tile": device},
            device_id_type=MESH,
        )

    for k in range(n - 1):
        window_copy(other(k), me).start()
    pltpu.make_async_copy(outgoing.at[me], gathered.at[me], recv_sem.at[mine]).start()

    def rounded(values):
        return values.astype(BF16).astype(F32)

    loads[-1].wait()

    row_angles, column_angles = row_phase[:, 0, :], column_phase[:, 0, :]
    for q, values in enumerate((
        jnp.cos(row_angles), jnp.sin(row_angles), jnp.cos(column_angles), jnp.sin(column_angles),
        row_bin[:, 0, :].astype(F32), column_bin[:, 0, :].astype(F32),
    )):
        values = values.reshape(groups, QUAD, LANES)
        waves[q, :, 0:QUAD] = values
        waves[q, :, QUAD:] = values
    octet_id = lax.broadcasted_iota(jnp.int32, (OCTET, LANES), 0)
    tiles = rows // OCTET

    pairs = [(a, t) for a in range(OCTET) for t in range(0, tiles, 2)]
    upper_half = octet_id >= QUAD
    second_row = jnp.where(upper_half, OCTET, 0)

    def spread(values, pattern):
        return pick(values, pattern)

    tables = []
    for group in range(groups):
        part = jnp.zeros((OCTET, LANES), F32)
        for i in range(QUAD):
            part = jnp.where(octet_id & (QUAD - 1) == i, fraction[0, group * QUAD + i], part)
        share[group] = part
        tables.append([rounded(waves[q, group]) for q in range(6)])
    column_bin_of = [table[5].astype(jnp.int32) for table in tables]
    for u, (a, t) in enumerate(pairs):
        pattern = second_row + (t * OCTET + a)
        turns = [(spread(table[0], pattern), spread(table[1], pattern)) for table in tables]
        offsets = [spread(table[4], pattern) for table in tables]
        for slot, ((cosine, sine), offset, table) in enumerate(zip(turns, offsets, tables)):
            column_cosine, column_sine = table[2], table[3]
            offset = offset.astype(jnp.int32)
            index_all[0, slot, u] = (offset + column_bin_of[slot]) & (LANES - 1)
            index_all[1, slot, u] = offset
            steer[0, slot, u] = cosine * column_cosine - sine * column_sine
            steer[1, slot, u] = cosine * column_sine + sine * column_cosine

    def profiles(group):
        for i in range(QUAD):
            values = gathered[group * QUAD + i].astype(F32)
            for j in (i, i + QUAD):
                windows[group, 4 * j : 4 * (j + 1), :] = values
        window = [windows[group, pl.ds(q, OCTET, stride=4), :] for q in range(4)]
        moved = [pltpu.roll(values, LANES - 1, 1) for values in window]
        fraction_of = share[group]
        profile = []
        for q in range(4):
            shifted = moved[q] if q % 2 else jnp.where(lane == LANES - 1, moved[q + 1], moved[q])
            profile.append(rounded((1.0 - fraction_of) * window[q] + fraction_of * shifted))
        return profile

    def contribute(group, profile, u):
        low = index_all[0, group, u]
        is_low = index_all[1, group, u] <= lane
        real = pick(jnp.where(is_low, profile[0], profile[1]), low)
        imag = pick(jnp.where(is_low, profile[2], profile[3]), low)
        turn_real, turn_imag = steer[0, group, u], steer[1, group, u]
        part_real = turn_real * real - turn_imag * imag
        part_imag = turn_real * imag + turn_imag * real
        a, t = pairs[u]
        top = pl.multiple_of(a * pair + group * OCTET, OCTET)
        both = (
            jnp.where(upper_half, pltpu.roll(part_imag, QUAD, 0), part_real),
            jnp.where(upper_half, part_imag, pltpu.roll(part_real, QUAD, 0)),
        )
        for h in range(2):
            left = (t + h) * LANES
            parts[pl.ds(top, OCTET), left : left + LANES] = both[h].astype(BF16)

    def arrive(slot):
        group = group_of(slot)
        arrived = gathered.at[pl.ds(group * QUAD, QUAD)]
        pltpu.make_async_copy(arrived, arrived, recv_sem.at[group]).wait()
        return group, profiles(group)

    def visit(slot, carry):
        group, profile = arrive(slot)
        for u in range(len(pairs)):
            contribute(group, profile, u)
        return carry

    lax.fori_loop(0, groups - 1, visit, 0)
    group, profile = arrive(groups - 1)
    grams = [jnp.zeros((pair, pair), F32)] * 2
    for a in range(OCTET):
        for u in range(a * tiles // 2, (a + 1) * tiles // 2):
            contribute(group, profile, u)
        half = tiles // 2 * LANES
        for h in range(2):
            values = parts[a * pair : (a + 1) * pair, h * half : (h + 1) * half]
            grams[h] = grams[h] + dot(values, values, ((1,), (1,)))
    gram = jnp.concatenate([grams[0] + grams[1], jnp.zeros((pair, LANES - pair), F32)], 1)
    folds = LANES // pair
    octets = n // OCTET

    def turned(values, shift):
        return pltpu.roll(values, shift % LANES, 1) if shift % LANES else values

    packed = [jnp.zeros((OCTET, LANES), F32)] * (-(-2 * octets // folds))
    for g in range(octets):
        first = gram[2 * g * OCTET : (2 * g + 1) * OCTET]
        second = gram[(2 * g + 1) * OCTET : (2 * g + 2) * OCTET]
        real = jnp.where(upper_half, pltpu.roll(second, QUAD, 0), first)
        imag = jnp.where(upper_half, second, pltpu.roll(first, QUAD, 0))
        for place in (g, octets + g):
            left = place % folds * pair
            if place == g:
                values = turned(real, left) + turned(imag, left - QUAD)
            else:
                values = turned(real, left - QUAD) - turned(imag, left)
            packed[place // folds] = jnp.where(lane & -pair == left, values, packed[place // folds])
    packed = jnp.concatenate([jnp.where((lane & QUAD) == 0, values, 0.0) for values in packed], 0)
    message[...] = packed
    messages[me] = packed

    def gram_copy(device, slot):
        return pltpu.make_async_remote_copy(
            src_ref=message,
            dst_ref=messages.at[slot],
            send_sem=send_sem2,
            recv_sem=recv_sem2,
            device_id={"tile": device},
            device_id_type=MESH,
        )

    for k in range(n - 1):
        gram_copy(other(k), me).start()
    sent = outgoing.at[pl.ds(0, n - 1)]
    pltpu.make_async_copy(sent, sent, send_sem).wait()
    sent = messages.at[pl.ds(0, n - 1)]
    pltpu.make_async_copy(sent, sent, recv_sem2).wait()

    total = jnp.sum(messages[...], axis=0)
    def along(values, axis):
        return jnp.sum(values, axis=axis, keepdims=True)

    inner = lane & (pair - 1)
    column_id = ((inner >> 1) & -QUAD) + (inner & (QUAD - 1))
    gram, near = [], []
    for place in range(2 * octets):
        top, left = place // folds * OCTET, place % folds * pair
        kept = column_id != octet_id + place % octets * OCTET
        values = jnp.where(kept, total[top : top + OCTET] * scale, 0.0)
        sums = along(jnp.where(lane & -pair == left, values, 0.0), 1)
        near.append(jnp.broadcast_to(sums, (OCTET, LANES)))
        gram.append(jnp.where(lane < pair, turned(values, -left), 0.0))
    gram_real, gram_imag = jnp.concatenate(gram[:octets], 0), jnp.concatenate(gram[octets:], 0)
    near_real, near_imag = jnp.concatenate(near[:octets], 0), jnp.concatenate(near[octets:], 0)
    mean = along(near_real * near_real + near_imag * near_imag, 0) / n
    one_real, one_imag = normalize(near_real, near_imag, mean)
    row_real, row_imag = normalize(along(gram_real, 0), -along(gram_imag, 0), mean)
    rest_real = along(gram_real * one_real + gram_imag * one_imag, 0)
    rest_imag = along(gram_real * one_imag - gram_imag * one_real, 0)
    again_real = row_real * rest_real + row_imag * rest_imag
    again_imag = row_real * rest_imag - row_imag * rest_real
    mean = jnp.broadcast_to(along(again_real * again_real + again_imag * again_imag, 1), (1, LANES)) / n
    two_real, two_imag = normalize(again_real, again_imag, mean)
    total_real = row_real * two_real - row_imag * two_imag
    total_imag = row_real * two_imag + row_imag * two_real
    lane_row = lax.broadcasted_iota(jnp.int32, total_real.shape, 1)
    own_lane = mine * 2 * QUAD + me % QUAD
    own = lane_row == own_lane
    correction[...] = jnp.concatenate([jnp.where(own, total_real, 0.0), jnp.where(own, total_imag, 0.0)], 0)
    weights = []
    for straight, crossed in ((total_real, -total_imag), (total_imag, total_real)):
        copies = []
        for left in range(0, LANES, pair):
            copies += [turned(straight * scale, left), turned(crossed * scale, left + QUAD)]
        while len(copies) > 1:
            copies = [x + y for x, y in zip(copies[::2], copies[1::2])]
        weights.append(jnp.broadcast_to(copies[0], (OCTET, LANES)))
    weights = jnp.concatenate(weights, 0)
    phase_id = lax.broadcasted_iota(jnp.int32, weights.shape, 0) & (OCTET - 1)
    weight_lane = lax.broadcasted_iota(jnp.int32, weights.shape, 1)
    spans = [
        jnp.where((weight_lane + left) & -pair == phase_id * pair, weights, 0.0) for left in range(0, OCTET * pair, LANES)
    ]
    weights = jnp.concatenate(spans, 1)
    high = weights.astype(BF16)
    low = (weights - high.astype(F32)).astype(BF16)
    weights = jnp.concatenate([high, low], 0)
    weights_out[...] = weights
    pltpu.make_async_copy(sent, sent, send_sem2).wait()


def image_kernel(parts, weights, correction_in, focused, correction, image, own, sem):
    copies = []
    step = 2 * LANES
    columns = parts.shape[1]
    chunks = 4
    for c in range(chunks):
        begin, end = c * columns // chunks, (c + 1) * columns // chunks
        for left in range(begin, end, step):
            both = dot(weights[...], parts[:, left : left + step])
            both = both[0 : 2 * OCTET] + both[2 * OCTET :]
            for i in range(step // LANES):
                top = (left // LANES + i) * OCTET
                for h in range(2):
                    image[h, 0, top : top + OCTET, :] = both[h * OCTET : (h + 1) * OCTET, i * LANES : (i + 1) * LANES]
        span = pl.ds(begin // LANES * OCTET, (end - begin) // LANES * OCTET)
        copy = pltpu.make_async_copy(image.at[:, :, span], focused.at[:, :, span], sem.at[c + 1])
        copy.start()
        copies.append(copy)
        if c == 0:
            sums = jnp.sum(correction_in[...], axis=1, keepdims=True)
            own[...] = jnp.concatenate([sums[0:1], sums[1:2]], 1)
            copies.append(pltpu.make_async_copy(own, correction, sem.at[0]))
            copies[-1].start()
    for copy in copies:
        copy.wait()


def solution(mesh):
    n = mesh.shape["tile"]

    def per_device(echoes, bin_start, bin_fraction, row_phase, column_phase, row_bin, column_bin):
        samples = echoes.shape[2]
        rows, columns = row_phase.shape[2], column_phase.shape[2]
        first, turn, last = tables(samples)
        bins = samples // LANES
        echo = echoes.reshape(2, bins, LANES)
        vmem = pl.BlockSpec(memory_space=pltpu.VMEM)
        operands = (
            bin_start, echo, jnp.asarray(first), jnp.asarray(turn), jnp.asarray(last),
            row_phase, column_phase, row_bin, column_bin, bin_fraction.T,
        )
        depth = -(-4 * n * n // (OCTET * LANES)) * OCTET
        parts, weights, correction = pl.pallas_call(
            functools.partial(kernel, n),
            out_shape=(
                pltpu.VMEM((OCTET * 2 * n, rows // OCTET * columns), BF16),
                pltpu.VMEM((4 * OCTET, OCTET * 2 * n), BF16),
                pltpu.VMEM((2, LANES), F32),
            ),
            in_specs=[pl.BlockSpec(memory_space=pltpu.HBM)] * len(operands),
            out_specs=(vmem, vmem, vmem),
            scratch_shapes=[pltpu.SMEM(bin_start.shape, jnp.int32)]
            + [pltpu.VMEM(operand.shape, operand.dtype) for operand in operands[1:9]]
            + [pltpu.SMEM((1, n), F32), pltpu.SemaphoreType.DMA((3,))]
            + [
                pltpu.VMEM((2, bins + OCTET, LANES), F32),
                pltpu.VMEM((n, 4, LANES), BF16),
                pltpu.VMEM((n, 4, LANES), BF16),
                pltpu.VMEM((6, n // QUAD, OCTET, LANES), F32),
                pltpu.VMEM((n // QUAD, OCTET, LANES), F32),
                pltpu.VMEM((2, n // QUAD, rows // 2, OCTET, LANES), jnp.int32),
                pltpu.VMEM((2, n // QUAD, rows // 2, OCTET, LANES), F32),
                pltpu.VMEM((n // QUAD, 4 * OCTET, LANES), F32),
                pltpu.VMEM((depth, LANES), F32),
                pltpu.VMEM((n, depth, LANES), F32),
                pltpu.SemaphoreType.DMA(()),
                pltpu.SemaphoreType.DMA((n // QUAD,)),
                pltpu.SemaphoreType.DMA(()),
                pltpu.SemaphoreType.DMA(()),
            ],
            compiler_params=pltpu.CompilerParams(collective_id=0, has_side_effects=True),
        )(*operands)
        hbm = pl.BlockSpec(memory_space=pltpu.HBM)
        focused, correction = pl.pallas_call(
            image_kernel,
            out_shape=(
                jax.ShapeDtypeStruct((2, 1, rows, columns), F32),
                jax.ShapeDtypeStruct((1, 2), F32),
            ),
            in_specs=[vmem] * 3,
            out_specs=(hbm, hbm),
            scratch_shapes=[
                pltpu.VMEM((2, 1, rows, columns), F32),
                pltpu.VMEM((1, 2), F32),
                pltpu.SemaphoreType.DMA((5,)),
            ],
        )(*[pltpu.with_memory_space_constraint(x, pltpu.VMEM) for x in (parts, weights, correction)])
        return focused, correction.T

    split = ("groups", "tile")
    in_specs = (
        P(None, split, None),
        P(split, None),
        P(None, split),
        P(None, split, None),
        P(None, split, None),
        P(None, split, None),
        P(None, split, None),
    )
    out_specs = (P(None, split, None, None), P(None, split))
    return jax.shard_map(per_device, mesh=mesh, in_specs=in_specs, out_specs=out_specs, check_vma=False)
```

```python
import functools
import math

import jax
import jax.numpy as jnp
import numpy as np
from jax import lax
from jax.experimental import pallas as pl
from jax.experimental.pallas import tpu as pltpu
from jax.sharding import PartitionSpec as P

LANES = 128
OCTET = 8
QUAD = 4
MESH = pl.DeviceIdType.MESH
F32 = jnp.float32
BF16 = jnp.bfloat16


def tables(samples):
    inner = LANES
    outer = samples // inner

    def wave(rows, columns, period):
        product = np.arange(rows)[:, None] * np.arange(columns)[None, :] % period
        phases = product * (2.0 * np.pi / period)
        return np.cos(phases), np.sin(phases)

    def split(table):
        table = table.astype(np.float32)
        high = table.astype(jnp.bfloat16)
        low = (table - high.astype(np.float32)).astype(jnp.bfloat16)
        return np.stack([high, low])

    first = split(np.concatenate(wave(outer, outer, outer), 1))
    last = split(np.concatenate(wave(inner, inner, inner), 1))
    turn = np.stack(wave(outer, inner, samples)) / math.sqrt(samples)
    return first, turn.astype(np.float32), last


def dot(a, b, dims=((1,), (0,)), precision=None):
    return lax.dot_general(a, b, (dims, ((), ())), precision=precision, preferred_element_type=F32)


def split3(table_ref, data, dims):
    high = data.astype(BF16)
    low = (data - high.astype(F32)).astype(BF16)
    return dot(table_ref[0], high, dims) + (dot(table_ref[1], high, dims) + dot(table_ref[0], low, dims))


def normalize(real_part, imag_part, mean):
    inverse = lax.rsqrt(real_part * real_part + imag_part * imag_part + mean + 1e-06)
    return real_part * inverse, imag_part * inverse


def pick(source, index):
    numbers = lax.GatherDimensionNumbers(
        offset_dims=(), collapsed_slice_dims=(1,), start_index_map=(1,),
        operand_batching_dims=(0,), start_indices_batching_dims=(0,),
    )
    return lax.gather(
        source, index[..., None], numbers, (1, 1), mode=lax.GatherScatterMode.PROMISE_IN_BOUNDS
    )


def kernel(
    n, starts_in, echo_in, first_in, turn_in, last_in, row_phase_in, column_phase_in, row_bin_in, column_bin_in,
    fraction_in,
    parts, weights_out, correction,
    starts, echo, first, turn, last, row_phase, column_phase, row_bin, column_bin, fraction, in_sem,
    spec, outgoing, gathered, waves, share, index_all, steer, windows,
    message, messages,
    send_sem, recv_sem, send_sem2, recv_sem2,
):
    me = lax.axis_index("tile")
    rows = row_phase.shape[2]
    scale = 1.0 / math.sqrt(n)
    groups = n // QUAD
    mine = me // QUAD
    pair = 2 * n

    barrier = pltpu.get_barrier_semaphore()
    for k in range(n - 1):
        place = (2 * me) // n * k + (1 - (2 * me) // n) * (n - 2 - k)
        far = place + (place >= me).astype(jnp.int32)
        pl.semaphore_signal(barrier, inc=1, device_id={"tile": far}, device_id_type=MESH)

    sources = (
        starts_in, echo_in, first_in, turn_in, last_in, row_phase_in, column_phase_in, row_bin_in, column_bin_in,
        fraction_in,
    )
    targets = (starts, echo, first, turn, last, row_phase, column_phase, row_bin, column_bin, fraction)
    last_load = len(sources) - 1
    loads = [
        pltpu.make_async_copy(source, target, in_sem.at[0 if i == 0 else 1 if i == last_load else 2])
        for i, (source, target) in enumerate(zip(sources, targets))
    ]
    for load in loads[1:] + loads[:1]:
        load.start()

    upper = (2 * me) // n

    def group_of(slot):
        place = upper * (groups - 1 - slot) + (1 - upper) * (slot - 1)
        place = place + (place >= mine).astype(jnp.int32)
        return place if isinstance(slot, int) else jnp.where(slot == 0, mine, place)

    def other(k):
        place = upper * k + (1 - upper) * (n - 2 - k)
        return place + (place >= me).astype(jnp.int32)


    size = sum(math.prod(target.shape) * target.dtype.itemsize for target in targets[1:-1])
    loaded = parts.at[pl.ds(0, size // (2 * parts.shape[1]))]
    pltpu.make_async_copy(loaded, loaded, in_sem.at[2]).wait()
    real, imag = echo[0], echo[1]
    data = jnp.concatenate(
        [jnp.concatenate([real, imag], 1), jnp.concatenate([imag, -real], 1)], 0
    )
    section = split3(first, data, ((1,), (0,)))
    half = section.shape[1] // 2
    real, imag = section[:, :half], section[:, half:]
    turned_real = real * turn[0] + imag * turn[1]
    turned_imag = imag * turn[0] - real * turn[1]
    data = jnp.concatenate(
        [jnp.concatenate([turned_real, turned_imag], 1), jnp.concatenate([turned_imag, -turned_real], 1)], 0
    )
    spectrum = split3(last, data, ((1,), (1,)))
    bins = spectrum.shape[0]
    spectrum = spectrum.astype(BF16).astype(F32)
    for h in range(2):
        spec[h, 0:bins, :] = spectrum[:, h * LANES : (h + 1) * LANES]
        spec[h, bins:, :] = jnp.zeros((spec.shape[1] - bins, LANES), F32)

    lane = lax.broadcasted_iota(jnp.int32, (OCTET, LANES), 1)
    loads[0].wait()
    for t in range(n):
        start = starts[0, t]
        top = start // LANES
        left = LANES - start % LANES
        pieces = []
        for h in range(2):
            moved = pltpu.roll(spec[h, pl.ds(top, OCTET), :], left % LANES, 1)
            below = pltpu.roll(moved, OCTET - 1, 0)
            pieces.append(jnp.where(lane < left, moved, below)[0:2])
        outgoing[t] = jnp.concatenate(pieces, 0).astype(BF16)

    pl.semaphore_wait(barrier, n - 1)

    def window_copy(device, slot):
        return pltpu.make_async_remote_copy(
            src_ref=outgoing.at[device],
            dst_ref=gathered.at[slot],
            send_sem=send_sem,
            recv_sem=recv_sem.at[slot // QUAD],
            device_id={"tile": device},
            device_id_type=MESH,
        )

    for k in range(n - 1):
        window_copy(other(k), me).start()
    pltpu.make_async_copy(outgoing.at[me], gathered.at[me], recv_sem.at[mine]).start()

    def rounded(values):
        return values.astype(BF16).astype(F32)

    loads[-1].wait()

    row_angles, column_angles = row_phase[:, 0, :], column_phase[:, 0, :]
    for q, values in enumerate((
        jnp.cos(row_angles), jnp.sin(row_angles), jnp.cos(column_angles), jnp.sin(column_angles),
        row_bin[:, 0, :].astype(F32), column_bin[:, 0, :].astype(F32),
    )):
        values = values.reshape(groups, QUAD, LANES)
        waves[q, :, 0:QUAD] = values
        waves[q, :, QUAD:] = values
    octet_id = lax.broadcasted_iota(jnp.int32, (OCTET, LANES), 0)
    tiles = rows // OCTET

    pairs = [(a, t) for a in range(OCTET) for t in range(0, tiles, 2)]
    upper_half = octet_id >= QUAD
    second_row = jnp.where(upper_half, OCTET, 0)

    def spread(values, pattern):
        return pick(values, pattern)

    tables = []
    for group in range(groups):
        part = jnp.zeros((OCTET, LANES), F32)
        for i in range(QUAD):
            part = jnp.where(octet_id & (QUAD - 1) == i, fraction[0, group * QUAD + i], part)
        share[group] = part
        tables.append([rounded(waves[q, group]) for q in range(6)])
    column_bin_of = [table[5].astype(jnp.int32) for table in tables]
    for u, (a, t) in enumerate(pairs):
        pattern = second_row + (t * OCTET + a)
        turns = [(spread(table[0], pattern), spread(table[1], pattern)) for table in tables]
        offsets = [spread(table[4], pattern) for table in tables]
        for slot, ((cosine, sine), offset, table) in enumerate(zip(turns, offsets, tables)):
            column_cosine, column_sine = table[2], table[3]
            offset = offset.astype(jnp.int32)
            index_all[0, slot, u] = (offset + column_bin_of[slot]) & (LANES - 1)
            index_all[1, slot, u] = offset
            steer[0, slot, u] = cosine * column_cosine - sine * column_sine
            steer[1, slot, u] = cosine * column_sine + sine * column_cosine

    def profiles(group):
        for i in range(QUAD):
            values = gathered[group * QUAD + i].astype(F32)
            for j in (i, i + QUAD):
                windows[group, 4 * j : 4 * (j + 1), :] = values
        window = [windows[group, pl.ds(q, OCTET, stride=4), :] for q in range(4)]
        moved = [pltpu.roll(values, LANES - 1, 1) for values in window]
        fraction_of = share[group]
        profile = []
        for q in range(4):
            shifted = moved[q] if q % 2 else jnp.where(lane == LANES - 1, moved[q + 1], moved[q])
            profile.append(rounded((1.0 - fraction_of) * window[q] + fraction_of * shifted))
        return profile

    def contribute(group, profile, u):
        low = index_all[0, group, u]
        is_low = index_all[1, group, u] <= lane
        real = pick(jnp.where(is_low, profile[0], profile[1]), low)
        imag = pick(jnp.where(is_low, profile[2], profile[3]), low)
        turn_real, turn_imag = steer[0, group, u], steer[1, group, u]
        part_real = turn_real * real - turn_imag * imag
        part_imag = turn_real * imag + turn_imag * real
        a, t = pairs[u]
        top = pl.multiple_of(a * pair + group * OCTET, OCTET)
        both = (
            jnp.where(upper_half, pltpu.roll(part_imag, QUAD, 0), part_real),
            jnp.where(upper_half, part_imag, pltpu.roll(part_real, QUAD, 0)),
        )
        for h in range(2):
            left = (t + h) * LANES
            parts[pl.ds(top, OCTET), left : left + LANES] = both[h].astype(BF16)

    def arrive(slot):
        group = group_of(slot)
        arrived = gathered.at[pl.ds(group * QUAD, QUAD)]
        pltpu.make_async_copy(arrived, arrived, recv_sem.at[group]).wait()
        return group, profiles(group)

    def visit(slot, carry):
        group, profile = arrive(slot)
        for u in range(len(pairs)):
            contribute(group, profile, u)
        return carry

    lax.fori_loop(0, groups - 1, visit, 0)
    group, profile = arrive(groups - 1)
    grams = [jnp.zeros((pair, pair), F32)] * 2
    for a in range(OCTET):
        for u in range(a * tiles // 2, (a + 1) * tiles // 2):
            contribute(group, profile, u)
        half = tiles // 2 * LANES
        for h in range(2):
            values = parts[a * pair : (a + 1) * pair, h * half : (h + 1) * half]
            grams[h] = grams[h] + dot(values, values, ((1,), (1,)))
    gram = jnp.concatenate([grams[0] + grams[1], jnp.zeros((pair, LANES - pair), F32)], 1)
    folds = LANES // pair
    octets = n // OCTET

    def turned(values, shift):
        return pltpu.roll(values, shift % LANES, 1) if shift % LANES else values

    packed = [jnp.zeros((OCTET, LANES), F32)] * (-(-2 * octets // folds))
    for g in range(octets):
        first = gram[2 * g * OCTET : (2 * g + 1) * OCTET]
        second = gram[(2 * g + 1) * OCTET : (2 * g + 2) * OCTET]
        real = jnp.where(upper_half, pltpu.roll(second, QUAD, 0), first)
        imag = jnp.where(upper_half, second, pltpu.roll(first, QUAD, 0))
        for place in (g, octets + g):
            left = place % folds * pair
            if place == g:
                values = turned(real, left) + turned(imag, left - QUAD)
            else:
                values = turned(real, left - QUAD) - turned(imag, left)
            packed[place // folds] = jnp.where(lane & -pair == left, values, packed[place // folds])
    packed = jnp.concatenate([jnp.where((lane & QUAD) == 0, values, 0.0) for values in packed], 0)
    message[...] = packed
    messages[me] = packed

    def gram_copy(device, slot):
        return pltpu.make_async_remote_copy(
            src_ref=message,
            dst_ref=messages.at[slot],
            send_sem=send_sem2,
            recv_sem=recv_sem2,
            device_id={"tile": device},
            device_id_type=MESH,
        )

    for k in range(n - 1):
        gram_copy(other(k), me).start()
    sent = outgoing.at[pl.ds(0, n - 1)]
    pltpu.make_async_copy(sent, sent, send_sem).wait()
    sent = messages.at[pl.ds(0, n - 1)]
    pltpu.make_async_copy(sent, sent, recv_sem2).wait()

    terms = [messages[i] for i in range(n)]
    while len(terms) > 1:
        terms = [x + y for x, y in zip(terms[::2], terms[1::2])]
    total = terms[0]
    def along(values, axis):
        return jnp.sum(values, axis=axis, keepdims=True)

    inner = lane & (pair - 1)
    column_id = ((inner >> 1) & -QUAD) + (inner & (QUAD - 1))
    gram, near = [], []
    for place in range(2 * octets):
        top, left = place // folds * OCTET, place % folds * pair
        kept = column_id != octet_id + place % octets * OCTET
        values = jnp.where(kept, total[top : top + OCTET] * scale, 0.0)
        sums = along(jnp.where(lane & -pair == left, values, 0.0), 1)
        near.append(jnp.broadcast_to(sums, (OCTET, LANES)))
        gram.append(jnp.where(lane < pair, turned(values, -left), 0.0))
    gram_real, gram_imag = jnp.concatenate(gram[:octets], 0), jnp.concatenate(gram[octets:], 0)
    near_real, near_imag = jnp.concatenate(near[:octets], 0), jnp.concatenate(near[octets:], 0)
    mean = along(near_real * near_real + near_imag * near_imag, 0) / n
    one_real, one_imag = normalize(near_real, near_imag, mean)
    row_real, row_imag = normalize(along(gram_real, 0), -along(gram_imag, 0), mean)
    rest_real = along(gram_real * one_real + gram_imag * one_imag, 0)
    rest_imag = along(gram_real * one_imag - gram_imag * one_real, 0)
    again_real = row_real * rest_real + row_imag * rest_imag
    again_imag = row_real * rest_imag - row_imag * rest_real
    mean = jnp.broadcast_to(along(again_real * again_real + again_imag * again_imag, 1), (1, LANES)) / n
    two_real, two_imag = normalize(again_real, again_imag, mean)
    total_real = row_real * two_real - row_imag * two_imag
    total_imag = row_real * two_imag + row_imag * two_real
    lane_row = lax.broadcasted_iota(jnp.int32, total_real.shape, 1)
    own_lane = mine * 2 * QUAD + me % QUAD
    own = lane_row == own_lane
    correction[...] = jnp.concatenate([jnp.where(own, total_real, 0.0), jnp.where(own, total_imag, 0.0)], 0)
    weights = []
    for straight, crossed in ((total_real, -total_imag), (total_imag, total_real)):
        copies = []
        for left in range(0, LANES, pair):
            copies += [turned(straight * scale, left), turned(crossed * scale, left + QUAD)]
        while len(copies) > 1:
            copies = [x + y for x, y in zip(copies[::2], copies[1::2])]
        weights.append(jnp.broadcast_to(copies[0], (OCTET, LANES)))
    weights = jnp.concatenate(weights, 0)
    phase_id = lax.broadcasted_iota(jnp.int32, weights.shape, 0) & (OCTET - 1)
    weight_lane = lax.broadcasted_iota(jnp.int32, weights.shape, 1)
    spans = [
        jnp.where((weight_lane + left) & -pair == phase_id * pair, weights, 0.0) for left in range(0, OCTET * pair, LANES)
    ]
    weights = jnp.concatenate(spans, 1)
    high = weights.astype(BF16)
    low = (weights - high.astype(F32)).astype(BF16)
    weights = jnp.concatenate([high, low], 0)
    weights_out[...] = weights
    pltpu.make_async_copy(sent, sent, send_sem2).wait()


def image_kernel(parts, weights, correction_in, focused, correction, image, own, sem):
    copies = []
    step = 2 * LANES
    columns = parts.shape[1]
    chunks = 4
    for c in range(chunks):
        begin, end = c * columns // chunks, (c + 1) * columns // chunks
        for left in range(begin, end, step):
            both = dot(weights[...], parts[:, left : left + step])
            both = both[0 : 2 * OCTET] + both[2 * OCTET :]
            for i in range(step // LANES):
                top = (left // LANES + i) * OCTET
                for h in range(2):
                    image[h, 0, top : top + OCTET, :] = both[h * OCTET : (h + 1) * OCTET, i * LANES : (i + 1) * LANES]
        span = pl.ds(begin // LANES * OCTET, (end - begin) // LANES * OCTET)
        copy = pltpu.make_async_copy(image.at[:, :, span], focused.at[:, :, span], sem.at[c + 1])
        copy.start()
        copies.append(copy)
        if c == 0:
            sums = jnp.sum(correction_in[...], axis=1, keepdims=True)
            own[...] = jnp.concatenate([sums[0:1], sums[1:2]], 1)
            copies.append(pltpu.make_async_copy(own, correction, sem.at[0]))
            copies[-1].start()
    for copy in copies:
        copy.wait()


def solution(mesh):
    n = mesh.shape["tile"]

    def per_device(echoes, bin_start, bin_fraction, row_phase, column_phase, row_bin, column_bin):
        samples = echoes.shape[2]
        rows, columns = row_phase.shape[2], column_phase.shape[2]
        first, turn, last = tables(samples)
        bins = samples // LANES
        echo = echoes.reshape(2, bins, LANES)
        vmem = pl.BlockSpec(memory_space=pltpu.VMEM)
        operands = (
            bin_start, echo, jnp.asarray(first), jnp.asarray(turn), jnp.asarray(last),
            row_phase, column_phase, row_bin, column_bin, bin_fraction.T,
        )
        depth = -(-4 * n * n // (OCTET * LANES)) * OCTET
        parts, weights, correction = pl.pallas_call(
            functools.partial(kernel, n),
            out_shape=(
                pltpu.VMEM((OCTET * 2 * n, rows // OCTET * columns), BF16),
                pltpu.VMEM((4 * OCTET, OCTET * 2 * n), BF16),
                pltpu.VMEM((2, LANES), F32),
            ),
            in_specs=[pl.BlockSpec(memory_space=pltpu.HBM)] * len(operands),
            out_specs=(vmem, vmem, vmem),
            scratch_shapes=[pltpu.SMEM(bin_start.shape, jnp.int32)]
            + [pltpu.VMEM(operand.shape, operand.dtype) for operand in operands[1:9]]
            + [pltpu.SMEM((1, n), F32), pltpu.SemaphoreType.DMA((3,))]
            + [
                pltpu.VMEM((2, bins + OCTET, LANES), F32),
                pltpu.VMEM((n, 4, LANES), BF16),
                pltpu.VMEM((n, 4, LANES), BF16),
                pltpu.VMEM((6, n // QUAD, OCTET, LANES), F32),
                pltpu.VMEM((n // QUAD, OCTET, LANES), F32),
                pltpu.VMEM((2, n // QUAD, rows // 2, OCTET, LANES), jnp.int32),
                pltpu.VMEM((2, n // QUAD, rows // 2, OCTET, LANES), F32),
                pltpu.VMEM((n // QUAD, 4 * OCTET, LANES), F32),
                pltpu.VMEM((depth, LANES), F32),
                pltpu.VMEM((n, depth, LANES), F32),
                pltpu.SemaphoreType.DMA(()),
                pltpu.SemaphoreType.DMA((n // QUAD,)),
                pltpu.SemaphoreType.DMA(()),
                pltpu.SemaphoreType.DMA(()),
            ],
            compiler_params=pltpu.CompilerParams(collective_id=0, has_side_effects=True),
        )(*operands)
        hbm = pl.BlockSpec(memory_space=pltpu.HBM)
        focused, correction = pl.pallas_call(
            image_kernel,
            out_shape=(
                jax.ShapeDtypeStruct((2, 1, rows, columns), F32),
                jax.ShapeDtypeStruct((1, 2), F32),
            ),
            in_specs=[vmem] * 3,
            out_specs=(hbm, hbm),
            scratch_shapes=[
                pltpu.VMEM((2, 1, rows, columns), F32),
                pltpu.VMEM((1, 2), F32),
                pltpu.SemaphoreType.DMA((5,)),
            ],
        )(*[pltpu.with_memory_space_constraint(x, pltpu.VMEM) for x in (parts, weights, correction)])
        return focused, correction.T

    split = ("groups", "tile")
    in_specs = (
        P(None, split, None),
        P(split, None),
        P(None, split),
        P(None, split, None),
        P(None, split, None),
        P(None, split, None),
        P(None, split, None),
    )
    out_specs = (P(None, split, None, None), P(None, split))
    return jax.shard_map(per_device, mesh=mesh, in_specs=in_specs, out_specs=out_specs, check_vma=False)
```
